32 devices in a mesh: zero: 8 (over y, x, core), tp: 4 (over z).
Axes of the slice: x: 2, y: 2, z: 4, core: 2. Of those that a mesh axis runs over, the one named last changes fastest.
Arguments:
- weight_gate: bfloat16 [2560, 9728], P('zero', 'tp'), may hold values from -0.125 to 0.125
- low_gate: bfloat16 [2560, 16], P('zero'), may hold values from -0.125 to 0.125
- high_gate: bfloat16 [16, 9728], P(None, 'tp'), may hold values from -1.5 to 1.5
- weight_up: bfloat16 [2560, 9728], P('zero', 'tp'), may hold values from -0.125 to 0.125
- low_up: bfloat16 [2560, 16], P('zero'), may hold values from -0.125 to 0.125
- high_up: bfloat16 [16, 9728], P(None, 'tp'), may hold values from -1.5 to 1.5
- weight_down: bfloat16 [9728, 2560], P('tp', 'zero'), may hold values from -0.0625 to 0.0625
- low_down: bfloat16 [9728, 16], P('tp'), may hold values from -0.0625 to 0.0625
- high_down: bfloat16 [16, 2560], P(None, 'zero'), may hold values from -1.5 to 1.5
- norm_train: float32 [2560], P(('zero', 'tp')), may hold values from 0.25 to 1.75
- norm_step: float32 [2560], P(('zero', 'tp')), may hold values from -0.3 to 0.3
Outputs:
- ready_gate: bfloat16 [2560, 9728], P(None, 'tp')
- ready_up: bfloat16 [2560, 9728], P(None, 'tp')
- ready_down: bfloat16 [9728, 2560], P('tp')
- serve_norm: bfloat16 [2560], replicated
The draws below stay inside these ranges and needn't reach their ends.
All inputs are finite; a program needn't handle non-finite values.
Results may differ from the reference program's by a relative error of at most 0.001.
Values may be sent and summed in bfloat16 or wider, within the bound.
A program may use at most 128 MiB of HBM per device.

```python
import jax
import jax.numpy as jnp

D_MODEL = 2560
D_INNER = 9728
RANK = 16


def shard_levels(own_key, dims, shards, low, top_value):
    def one(dim, parts):
        steps = jax.random.uniform(jax.random.fold_in(jax.random.fold_in(own_key, 6), dim), (parts,), jnp.float32, low / len(shards), top_value / len(shards))
        return jnp.repeat(jnp.exp(steps), dims[dim] // parts).reshape((-1,) + (1,) * (len(dims) - dim - 1))

    loudness = one(*shards[0])
    for cut in shards[1:]:
        loudness = loudness * one(*cut)
    return loudness


def gaussian(stream_key, shape, spread, most, shards=(), kind=jnp.bfloat16):
    array = jax.random.normal(stream_key, shape, jnp.float32) * spread
    if len(shards) > 0:
        array = shard_levels(stream_key, shape, shards, -0.22, 0.18) * array
    return jnp.clip(array, min=-most, max=most).astype(kind)


def setup_inputs(seed: int = 0) -> dict:
    key_of = jax.random.split(jax.random.key(seed), 12)
    return {
        "weight_gate": gaussian(key_of[0], (D_MODEL, D_INNER), D_MODEL ** -0.5, 0.125, ((0, 8), (1, 4))),
        "low_gate": gaussian(key_of[1], (D_MODEL, RANK), D_MODEL ** -0.5, 0.125, ((0, 8),)),
        "high_gate": gaussian(key_of[2], (RANK, D_INNER), RANK ** -0.5, 1.5, ((1, 4),)),
        "weight_up": gaussian(key_of[3], (D_MODEL, D_INNER), D_MODEL ** -0.5, 0.125, ((0, 8), (1, 4))),
        "low_up": gaussian(key_of[4], (D_MODEL, RANK), D_MODEL ** -0.5, 0.125, ((0, 8),)),
        "high_up": gaussian(key_of[5], (RANK, D_INNER), RANK ** -0.5, 1.5, ((1, 4),)),
        "weight_down": gaussian(key_of[6], (D_INNER, D_MODEL), D_INNER ** -0.5, 0.0625, ((0, 4), (1, 8))),
        "low_down": gaussian(key_of[7], (D_INNER, RANK), D_INNER ** -0.5, 0.0625, ((0, 4),)),
        "high_down": gaussian(key_of[8], (RANK, D_MODEL), RANK ** -0.5, 1.5, ((1, 8),)),
        "norm_train": jnp.clip(1.0 + 0.15 * jax.random.normal(key_of[9], (D_MODEL,), jnp.float32), 0.25, 1.75),
        "norm_step": jnp.clip(jax.random.uniform(key_of[10], (D_MODEL,), jnp.float32, -0.3, 0.3) * shard_levels(key_of[10], (D_MODEL,), ((0, 32),), -0.4, 0.0), -0.3, 0.3),
    }


mix_rate = 0.5


def reference(weight_gate, low_gate, high_gate, weight_up, low_up, high_up, weight_down, low_down, high_down, norm_train, norm_step):
    latest_gate = weight_gate.astype(jnp.float32) + mix_rate * jnp.dot(low_gate, high_gate, preferred_element_type=jnp.float32)
    latest_up = weight_up.astype(jnp.float32) + mix_rate * jnp.dot(low_up, high_up, preferred_element_type=jnp.float32)
    latest_down = weight_down.astype(jnp.float32) + mix_rate * jnp.dot(low_down, high_down, preferred_element_type=jnp.float32)
    ready_gate = latest_gate.astype(jnp.bfloat16)
    ready_up = latest_up.astype(jnp.bfloat16)
    ready_down = latest_down.astype(jnp.bfloat16)
    serve_norm = (norm_train + norm_step).astype(jnp.bfloat16)
    return ready_gate, ready_up, ready_down, serve_norm
```

```python
import functools

import jax
import jax.numpy as jnp
from jax import lax
from jax.experimental import pallas as pl
from jax.experimental.pallas import tpu as pltpu
from jax.sharding import PartitionSpec as P

mix_rate = 0.5
MESH = pl.DeviceIdType.MESH
LANES = 128
CHUNKS = 4
HALF = CHUNKS // 2
GROUP = 8
GRANT = 32 * 2**20
VMEM = pl.BlockSpec(memory_space=pltpu.VMEM)
ANY = pl.BlockSpec(memory_space=pl.ANY)
EARLY, LATE = range(HALF), range(HALF, CHUNKS)


def merge_rows(weight, factor, other):
    product = lax.dot_general(
        factor, other, (((0,), (0,)), ((), ())), preferred_element_type=jnp.float32
    )
    return (weight.astype(jnp.float32) + mix_rate * product).astype(jnp.bfloat16)


class Place:
    def __init__(self):
        me = lax.axis_index("zero")
        core = lax.rem(me, 2)
        x = lax.rem(lax.div(me, 2), 2)
        y = lax.div(me, 4)

        def at(yy, xx, cc):
            return (yy * 2 + xx) * 2 + cc

        self.me, self.core = me, core
        self.partner = at(y, x, 1 - core)
        self.across_x = at(y, 1 - x, core)
        self.across_y = at(1 - y, x, core)
        self.across = at(1 - y, 1 - x, core)
        self.group = [
            at(
                y + dy - 2 * y * dy,
                x + dx - 2 * x * dx,
                core + dc - 2 * core * dc,
            )
            for dy in (0, 1) for dx in (0, 1) for dc in (0, 1) if dy + dx + dc
        ]

    def other_core(self, owner):
        return owner + self.partner - self.me


def remote(src, dst, peer, send, recv):
    return pltpu.make_async_remote_copy(
        src_ref=src, dst_ref=dst, send_sem=send, recv_sem=recv,
        device_id={"zero": peer}, device_id_type=MESH,
    )


def first_kernel(
    tp,
    weight_down, factor_down, other_down,
    weight_gate, factor_gate, other_gate,
    weight_up, factor_up, other_up,
    norm_train, norm_step,
    gate, down, extra, gains, held, weights, w_sems,
    n_send, n_recv,
    x_send, x_recv, y_send, y_recv, fx_send, fx_recv, fy_send, fy_recv, p_send, p_recv,
    ex_send, ex_recv, ey_send, ey_recv,
):
    rows, columns = weight_gate.shape
    step = rows // CHUNKS
    z = Place()
    me = z.me

    loads = [
        pltpu.make_async_copy(weight, weights.at[i], w_sems.at[i])
        for i, weight in enumerate((weight_down, weight_gate, weight_up))
    ]
    for load in loads:
        load.start()

    mine = lax.axis_index("tp")
    peers, width = [{"zero": peer} for peer in z.group], 1
    while width < tp:
        bit = lax.rem(lax.div(mine, width), 2)
        peers.append({"tp": mine + width - 2 * width * bit})
        width *= 2

    barrier = pltpu.get_barrier_semaphore()
    for peer in peers:
        pl.semaphore_signal(barrier, inc=1, device_id=peer, device_id_type=MESH)
    place = mine * GROUP + me
    size = norm_train.shape[1]
    gains[place, :, 0:size] = norm_train[...] + norm_step[...]

    stacks = (held, gate)
    factors = (
        (factor_down, other_down), (factor_gate, other_gate), (factor_up, other_up)
    )

    def merge(i, c):
        factor, other = factors[i]
        first = c * step

        @pl.loop(0, columns // LANES)
        def _(t):
            cols = pl.ds(pl.multiple_of(t * LANES, LANES), LANES)
            block = merge_rows(
                weights[i, pl.ds(first, step), cols],
                factor[:, pl.ds(first, step)],
                other[:, cols],
            )
            if i < 2:
                stacks[i][pl.ds(pl.multiple_of(me * rows + first, 16), step), cols] = block
            else:
                extra[0, pl.ds(first, step), cols] = block

    loads[0].wait()
    merge(0, 0)
    pl.semaphore_wait(barrier, len(peers))

    def pass_gains(k, first, count):
        block = gains.at[pl.ds(first, count)]
        dma = pltpu.make_async_remote_copy(
            src_ref=block, dst_ref=block, send_sem=n_send.at[k], recv_sem=n_recv.at[k],
            device_id=peers[k], device_id_type=MESH,
        )
        dma.start()
        return dma

    def copy(i, owner, c, peer, send, recv):
        first = pl.multiple_of(owner * rows + c * step, 16)
        ref = stacks[i].at[pl.ds(first, step), :]
        return remote(ref, ref, peer, send, recv)

    def on_x(i, owner, c):
        return copy(i, owner, c, z.across_x, x_send.at[i, c], x_recv.at[i, c])

    def on_y(i, owner, c):
        return copy(i, owner, c, z.across_y, y_send.at[i, c], y_recv.at[i, c])

    def forward_x(i, owner, c):
        return copy(i, owner, c, z.across_x, fx_send.at[i, c - HALF], fx_recv.at[i, c - HALF])

    def forward_y(i, owner, c):
        return copy(i, owner, c, z.across_y, fy_send.at[i, c], fy_recv.at[i, c])

    def share(i, slot, owner, c):
        return copy(i, owner, c, z.partner, p_send.at[slot, i, c], p_recv.at[slot, i, c])

    def ahead_x(c):
        at = pl.ds(c * step, step)
        return remote(
            extra.at[0, at], extra.at[1, at], z.across_x, ex_send.at[c], ex_recv.at[c]
        )

    def ahead_y(c):
        at = pl.ds(c * step, step)
        return remote(
            extra.at[0, at], extra.at[2, at], z.across_y, ey_send.at[c], ey_recv.at[c]
        )

    sent = []

    def go(dma):
        dma.start()
        sent.append(dma)

    go(on_x(0, me, 0))
    passed = [pass_gains(k, place, 1) for k in range(len(z.group))]
    for i in range(2):
        if i:
            loads[i].wait()
        for c, d in zip(EARLY, LATE):
            if i or c:
                merge(i, c)
                go(on_x(i, me, c))
            merge(i, d)
            go(on_y(i, me, d))
        for c, d in zip(EARLY, LATE):
            go(on_x(i, me, d))
            go(on_y(i, me, c))
        for c in range(CHUNKS):
            go(share(i, 0, me, c))
    loads[2].wait()
    for c in range(CHUNKS):
        merge(2, c)

    for dma in passed:
        dma.wait_recv()
    for k in range(len(z.group), len(peers)):
        width = 1 << (k - len(z.group))
        passed.append(pass_gains(k, lax.div(mine, width) * (width * GROUP), width * GROUP))
        passed[-1].wait_recv()
    sent += passed

    def turn(owner):
        base = pl.multiple_of(lax.div(owner, 2) * (2 * rows), LANES)

        @pl.loop(0, columns // LANES)
        def _(t):
            cols = pl.ds(pl.multiple_of(t * LANES, LANES), LANES)
            down[cols, pl.ds(base, 2 * rows)] = held[pl.ds(base, 2 * rows), cols].T

    def shared(i, slot, owner):
        for c in range(CHUNKS):
            share(i, slot, z.other_core(owner), c).wait_recv()

    for i in range(2):
        for c, d in zip(EARLY, LATE):
            on_x(i, z.across_x, c).wait_recv()
            go(forward_y(i, z.across_x, c))
            go(share(i, 1, z.across_x, c))
            on_y(i, z.across_y, d).wait_recv()
            go(forward_x(i, z.across_y, d))
            go(share(i, 2, z.across_y, d))
        if i == 1:
            @pl.when(z.core == 1)
            def _():
                for c, d in zip(EARLY, LATE):
                    ahead_x(c).start()
                    ahead_y(d).start()
                for c, d in zip(EARLY, LATE):
                    ahead_x(d).start()
                    ahead_y(c).start()
        for c, d in zip(EARLY, LATE):
            on_x(i, z.across_x, d).wait_recv()
            go(share(i, 1, z.across_x, d))
            on_y(i, z.across_y, c).wait_recv()
            go(share(i, 2, z.across_y, c))
        for slot, owner in ((0, me), (1, z.across_x), (2, z.across_y)):
            shared(i, slot, owner)
            if i == 0:
                turn(owner)
    for i in range(2):
        for c, d in zip(EARLY, LATE):
            forward_y(i, z.across, c).wait_recv()
            go(share(i, 3, z.across, c))
            forward_x(i, z.across, d).wait_recv()
            go(share(i, 3, z.across, d))
        if i == 0:
            shared(i, 3, z.across)
            turn(z.across)
    shared(1, 3, z.across)
    for dma in sent:
        dma.wait_send()

    @pl.when(z.core == 1)
    def _():
        for c in range(CHUNKS):
            ahead_x(c).wait()
            ahead_y(c).wait()


def first(sources, norms, tp):
    rows, columns = sources[0].shape
    stack = (rows * GROUP, columns)
    turned = (columns, rows * GROUP)
    dma = pltpu.SemaphoreType.DMA
    stages = GROUP - 1 + tp.bit_length() - 1
    return pl.pallas_call(
        functools.partial(first_kernel, tp),
        out_shape=(
            pltpu.VMEM(stack, jnp.bfloat16),
            pltpu.VMEM(turned, jnp.bfloat16),
            pltpu.VMEM((3, rows, columns), jnp.bfloat16),
            pltpu.VMEM((GROUP * tp, 1, LANES), jnp.float32),
        ),
        in_specs=[ANY, VMEM, VMEM] * 3 + [VMEM, VMEM],
        out_specs=[VMEM] * 4,
        scratch_shapes=[
            pltpu.VMEM(stack, jnp.bfloat16),
            pltpu.VMEM((3, rows, columns), jnp.bfloat16),
            dma((3,)),
            dma((stages,)), dma((stages,)),
            dma((2, CHUNKS)), dma((2, CHUNKS)), dma((2, CHUNKS)), dma((2, CHUNKS)),
            dma((2, HALF)), dma((2, HALF)), dma((2, HALF)), dma((2, HALF)),
            dma((4, 2, CHUNKS)), dma((4, 2, CHUNKS)),
            dma((CHUNKS,)), dma((CHUNKS,)), dma((CHUNKS,)), dma((CHUNKS,)),
        ],
        compiler_params=pltpu.CompilerParams(
            collective_id=0, has_side_effects=True, vmem_limit_bytes=GRANT
        ),
        name="gather_first",
    )(*sources, *norms)


def second_kernel(
    extra, after, up, ready, l_sems,
    x_send, x_recv, y_send, y_recv, fx_send, fx_recv, fy_send, fy_recv, p_send, p_recv,
):
    _, rows, columns = extra.shape
    step = rows // CHUNKS
    z = Place()
    me = z.me

    barrier = pltpu.get_barrier_semaphore()
    for peer in (z.across_x, z.across_y):
        pl.semaphore_signal(barrier, inc=1, device_id={"zero": peer}, device_id_type=MESH)

    @pl.when(z.core == 0)
    def _():
        pl.semaphore_signal(
            barrier, inc=1, device_id={"zero": z.partner}, device_id_type=MESH
        )

    pl.semaphore_wait(barrier, 2 + z.core)

    def part(owner, c):
        return up.at[pl.ds(pl.multiple_of(owner * rows + c * step, 16), step), :]

    def kept(slot, c):
        return extra.at[slot, pl.ds(c * step, step)]

    def on_x(c):
        return remote(kept(0, c), part(me, c), z.across_x, x_send.at[c], x_recv.at[c])

    def on_y(c):
        return remote(kept(0, c), part(me, c), z.across_y, y_send.at[c], y_recv.at[c])

    def forward_x(src, c):
        return remote(
            src, part(z.across_y, c), z.across_x, fx_send.at[c - HALF], fx_recv.at[c - HALF]
        )

    def forward_y(src, c):
        return remote(src, part(z.across_x, c), z.across_y, fy_send.at[c], fy_recv.at[c])

    def share(src, slot, owner, c):
        return remote(src, part(owner, c), z.partner, p_send.at[slot, c], p_recv.at[slot, c])

    def move(slot, owner):
        at = pl.ds(pl.multiple_of(owner * rows, 16), rows)
        return pltpu.make_async_copy(extra.at[slot], up.at[at, :], l_sems.at[slot])

    owners = (me, z.across_x, z.across_y)

    @pl.when(z.core == 0)
    def _():
        for c, d in zip(EARLY, LATE):
            on_x(c).start()
            on_y(d).start()
        for c, d in zip(EARLY, LATE):
            on_x(d).start()
            on_y(c).start()
        move(0, me).start()
        for c, d in zip(EARLY, LATE):
            on_x(c).wait_recv()
            forward_y(part(z.across_x, c), c).start()
            on_y(d).wait_recv()
            forward_x(part(z.across_y, d), d).start()
        for c, d in zip(EARLY, LATE):
            on_x(d).wait_recv()
            on_y(c).wait_recv()
        pl.semaphore_wait(ready, 1)
        for c in range(CHUNKS):
            share(kept(0, c), 0, me, c).start()
        for slot in (1, 2):
            for c in range(CHUNKS):
                share(part(owners[slot], c), slot, owners[slot], c).start()
        for c in range(CHUNKS):
            on_x(c).wait_send()
            on_y(c).wait_send()
        move(0, me).wait()

    @pl.when(z.core == 1)
    def _():
        pl.semaphore_signal(
            ready, inc=1, device_id={"zero": z.partner}, device_id_type=MESH
        )
        for c, d in zip(EARLY, LATE):
            forward_y(kept(1, c), c).start()
            forward_x(kept(2, d), d).start()
        for slot, owner in enumerate(owners):
            for c in range(CHUNKS):
                share(kept(slot, c), slot, owner, c).start()
        for slot, owner in enumerate(owners):
            move(slot, owner).start()
        for slot, owner in enumerate(owners):
            move(slot, owner).wait()

    for c, d in zip(EARLY, LATE):
        forward_y(kept(1, c), c).wait_recv()
        share(part(z.across, c), 3, z.across, c).start()
        forward_x(kept(2, d), d).wait_recv()
        share(part(z.across, d), 3, z.across, d).start()
    for slot, owner in enumerate((*owners, z.across)):
        for c in range(CHUNKS):
            share(part(owner, c), slot, z.other_core(owner), c).wait()
    for c, d in zip(EARLY, LATE):
        forward_y(kept(1, c), c).wait_send()
        forward_x(kept(2, d), d).wait_send()


def second(extra, after):
    _, rows, columns = extra.shape
    dma = pltpu.SemaphoreType.DMA
    extra = pltpu.with_memory_space_constraint(extra, pltpu.VMEM)
    return pl.pallas_call(
        second_kernel,
        out_shape=pltpu.VMEM((rows * GROUP, columns), jnp.bfloat16),
        in_specs=[VMEM, ANY],
        out_specs=VMEM,
        scratch_shapes=[
            pltpu.SemaphoreType.REGULAR,
            dma((3,)),
            dma((CHUNKS,)), dma((CHUNKS,)), dma((CHUNKS,)), dma((CHUNKS,)),
            dma((HALF,)), dma((HALF,)), dma((HALF,)), dma((HALF,)),
            dma((4, CHUNKS)), dma((4, CHUNKS)),
        ],
        compiler_params=pltpu.CompilerParams(
            collective_id=1, has_side_effects=True, vmem_limit_bytes=2**20
        ),
        name="gather_second",
    )(extra, after)


def start_stores(sources, targets, sems):
    pieces = 4
    copies = []
    for i, (src, dst) in enumerate(zip(sources, targets)):
        size = src.shape[0] // pieces
        for k in range(pieces):
            at = pl.ds(k * size, size)
            copies.append(pltpu.make_async_copy(src.at[at], dst.at[at], sems.at[i, k]))
            copies[-1].start()
    return copies


def store_kernel(count, *refs):
    for copy in start_stores(refs[:count], refs[count:-1], refs[-1]):
        copy.wait()


def store_norm_kernel(tp, size, gate, down, gains, gate_out, down_out, norm, lines, sems):
    copies = start_stores((gate, down), (gate_out, down_out), sems)
    lane = lax.broadcasted_iota(jnp.int32, (1, LANES), 1)
    parts = [[] for _ in range(lines.shape[0])]
    for k in range(GROUP * tp):
        zero, z = divmod(k, tp)
        piece = jnp.where(lane < size, gains[z * GROUP + zero], 0.0)
        line, shift = divmod(k * size, LANES)
        piece = pltpu.roll(piece, shift, 1) if shift else piece
        parts[line].append(jnp.where(lane >= shift, piece, 0.0))
        if shift + size > LANES:
            parts[line + 1].append(jnp.where(lane < shift, piece, 0.0))
    for line, terms in enumerate(parts):
        lines[pl.ds(line, 1), :] = sum(terms[1:], terms[0])
    norm[...] = lines[...].astype(jnp.bfloat16)
    for copy in copies:
        copy.wait()


def in_vmem(*arrays):
    return [pltpu.with_memory_space_constraint(a, pltpu.VMEM) for a in arrays]


def store(*held):
    held = in_vmem(*held)
    return pl.pallas_call(
        functools.partial(store_kernel, len(held)),
        out_shape=tuple(jax.ShapeDtypeStruct(a.shape, a.dtype) for a in held),
        in_specs=[VMEM] * len(held),
        out_specs=[ANY] * len(held),
        scratch_shapes=[pltpu.SemaphoreType.DMA((len(held), 4))],
        compiler_params=pltpu.CompilerParams(vmem_limit_bytes=2**20),
        name="store_merged",
    )(*held)


def store_norm(gate, down, gains, tp, size):
    held = in_vmem(gate, down, gains)
    lines = (GROUP * tp * size // LANES, LANES)
    shapes = [jax.ShapeDtypeStruct(a.shape, a.dtype) for a in held[:2]]
    return pl.pallas_call(
        functools.partial(store_norm_kernel, tp, size),
        out_shape=(*shapes, jax.ShapeDtypeStruct(lines, jnp.bfloat16)),
        in_specs=[VMEM] * 3,
        out_specs=[ANY, ANY, VMEM],
        scratch_shapes=[pltpu.VMEM(lines, jnp.float32), pltpu.SemaphoreType.DMA((2, 4))],
        compiler_params=pltpu.CompilerParams(vmem_limit_bytes=2**20),
        name="store_first",
    )(*held)


def local(
    weight_gate, low_gate, high_gate,
    weight_up, low_up, high_up,
    weight_down, low_down, high_down,
    norm_train, norm_step,
    *, fast, tp,
):
    sources = (
        (weight_down.T, high_down, low_down.T),
        (weight_gate, low_gate.T, high_gate),
        (weight_up, low_up.T, high_up),
    )
    if fast:
        norms = (norm_train[None], norm_step[None])
        gate, down, extra, gains = first(sum(sources, ()), norms, tp)
        ready_gate, ready_down, norm = store_norm(gate, down, gains, tp, norm_train.shape[0])
        (ready_up,) = store(second(extra, norm))
        serve_norm = norm.reshape(-1)
    else:
        down, gate, up = (merge_rows(*s) for s in sources)
        ready_gate, ready_up, ready_down = (
            lax.all_gather(a, "zero", axis=0, tiled=True) for a in (gate, up, down)
        )
        ready_down = ready_down.T
        serve_norm = lax.all_gather(
            (norm_train + norm_step).astype(jnp.bfloat16), ("zero", "tp"), axis=0, tiled=True
        )
    return (ready_gate, ready_up, ready_down, serve_norm)


def solution(mesh):
    def step(*args):
        zero, tp = mesh.shape["zero"], mesh.shape["tp"]
        rows, columns = args[0].shape[0] // zero, args[0].shape[1] // tp
        fast = (
            zero == GROUP
            and tp & (tp - 1) == 0
            and args[9].shape[0] <= zero * tp * LANES
            and args[9].shape[0] % LANES == 0
            and rows % (16 * CHUNKS) == 0
            and columns % LANES == 0
            and 2 * rows % LANES == 0
            and args[6].shape == args[0].shape[::-1]
        )
        return jax.shard_map(
            functools.partial(local, fast=fast, tp=tp),
            mesh=mesh,
            in_specs=(
                P("zero", "tp"), P("zero", None), P(None, "tp"),
                P("zero", "tp"), P("zero", None), P(None, "tp"),
                P("tp", "zero"), P("tp", None), P(None, "zero"),
                P(("zero", "tp")), P(("zero", "tp")),
            ),
            out_specs=(P(None, "tp"), P(None, "tp"), P("tp", None), P()),
            check_vma=False,
        )(*args)

    return step
```

```python
import functools

import jax
import jax.numpy as jnp
from jax import lax
from jax.experimental import pallas as pl
from jax.experimental.pallas import tpu as pltpu
from jax.sharding import PartitionSpec as P

mix_rate = 0.5
MESH = pl.DeviceIdType.MESH
LANES = 128
TILE = 2 * LANES
CHUNKS = 4
HALF = CHUNKS // 2
GROUP = 8
GRANT = 32 * 2**20
VMEM = pl.BlockSpec(memory_space=pltpu.VMEM)
ANY = pl.BlockSpec(memory_space=pl.ANY)
EARLY, LATE = range(HALF), range(HALF, CHUNKS)
FIRST = [c for pair in zip(EARLY, LATE) for c in pair]


def merged(weight, product):
    return (weight.astype(jnp.float32) + mix_rate * product).astype(jnp.bfloat16)


def merge_rows(weight, factor, other):
    product = lax.dot_general(
        factor, other, (((0,), (0,)), ((), ())), preferred_element_type=jnp.float32
    )
    return merged(weight, product)


class Place:
    def __init__(self):
        me = lax.axis_index("zero")
        core = lax.rem(me, 2)
        x = lax.rem(lax.div(me, 2), 2)
        y = lax.div(me, 4)

        def at(yy, xx, cc):
            return (yy * 2 + xx) * 2 + cc

        self.me, self.core = me, core
        self.partner = at(y, x, 1 - core)
        self.across_x = at(y, 1 - x, core)
        self.across_y = at(1 - y, x, core)
        self.across = at(1 - y, 1 - x, core)
        self.group = [
            at(
                y + dy - 2 * y * dy,
                x + dx - 2 * x * dx,
                core + dc - 2 * core * dc,
            )
            for dy in (0, 1) for dx in (0, 1) for dc in (0, 1) if dy + dx + dc
        ]

    def other_core(self, owner):
        return owner + self.partner - self.me


def remote(src, dst, peer, send, recv):
    return pltpu.make_async_remote_copy(
        src_ref=src, dst_ref=dst, send_sem=send, recv_sem=recv,
        device_id={"zero": peer}, device_id_type=MESH,
    )


def first_kernel(
    tp,
    weight_down, factor_down, other_down,
    weight_gate, factor_gate, other_gate,
    weight_up, factor_up, other_up,
    norm_train, norm_step,
    gate, down, extra, gains, held, weights, lefts, rights, norms, w_sems,
    n_send, n_recv,
    x_send, x_recv, y_send, y_recv, fx_send, fx_recv, fy_send, fy_recv, p_send, p_recv,
    ex_send, ex_recv, ey_send, ey_recv,
):
    rows, columns = weight_gate.shape
    step = rows // CHUNKS
    z = Place()
    me = z.me

    mine = lax.axis_index("tp")
    peers, width = [{"zero": peer} for peer in z.group], 1
    while width < tp:
        bit = lax.rem(lax.div(mine, width), 2)
        peers.append({"tp": mine + width - 2 * width * bit})
        width *= 2

    barrier = pltpu.get_barrier_semaphore()
    for peer in peers:
        pl.semaphore_signal(barrier, inc=1, device_id=peer, device_id_type=MESH)

    loads = []

    def load(src, dst):
        loads.append(pltpu.make_async_copy(src, dst, w_sems.at[len(loads)]))
        loads[-1].start()
        return loads[-1]

    wide = ((weight_down, factor_down, other_down), (weight_gate, factor_gate, other_gate),
            (weight_up, factor_up, other_up))
    narrow = [[load(factor, lefts.at[0]), load(other, rights.at[0])]
              for _, factor, other in wide[:1]]
    pieces = [[load(wide[0][0].at[pl.ds(c * step, step)], weights.at[0, pl.ds(c * step, step)])
               for c in FIRST]]
    norm_loads = [load(norm_train, norms.at[0]), load(norm_step, norms.at[1])]
    for i in (1, 2):
        weight, factor, other = wide[i]
        narrow.append([load(factor, lefts.at[i]), load(other, rights.at[i])])
        pieces.append([load(weight, weights.at[i])])

    stacks = (held, gate)

    turned = [None] * 3

    def merge(i, c):
        other = rights.at[i]
        if turned[i] is None:
            for dma in narrow[i]:
                dma.wait()
            turned[i] = lefts[i].T
        if i == 0:
            pieces[0][FIRST.index(c)].wait()
        elif c == 0:
            pieces[i][0].wait()
        lhs = turned[i][c * step:(c + 1) * step]
        here = pl.ds(c * step, step)
        for t in range(0, columns, TILE):
            cols = pl.ds(t, min(TILE, columns - t))
            product = jnp.dot(lhs, other[:, cols], preferred_element_type=jnp.float32)
            block = merged(weights[i, here, cols], product)
            if i < 2:
                own = pl.ds(pl.multiple_of(me * rows + c * step, 16), step)
                stacks[i][own, cols] = block
            else:
                extra[0, here, cols] = block

    merge(0, 0)
    merge(0, HALF)
    pl.semaphore_wait(barrier, len(peers))

    def pass_gains(k, first, count):
        block = gains.at[pl.ds(first, count)]
        dma = pltpu.make_async_remote_copy(
            src_ref=block, dst_ref=block, send_sem=n_send.at[k], recv_sem=n_recv.at[k],
            device_id=peers[k], device_id_type=MESH,
        )
        dma.start()
        return dma

    def copy(i, owner, c, peer, send, recv):
        first = pl.multiple_of(owner * rows + c * step, 16)
        ref = stacks[i].at[pl.ds(first, step), :]
        return remote(ref, ref, peer, send, recv)

    def on_x(i, owner, c):
        return copy(i, owner, c, z.across_x, x_send.at[i, c], x_recv.at[i, c])

    def on_y(i, owner, c):
        return copy(i, owner, c, z.across_y, y_send.at[i, c], y_recv.at[i, c])

    def forward_x(i, owner, c):
        return copy(i, owner, c, z.across_x, fx_send.at[i, c - HALF], fx_recv.at[i, c - HALF])

    def forward_y(i, owner, c):
        return copy(i, owner, c, z.across_y, fy_send.at[i, c], fy_recv.at[i, c])

    def share(i, slot, owner, c):
        return copy(i, owner, c, z.partner, p_send.at[slot, i, c], p_recv.at[slot, i, c])

    def ahead_x(c):
        at = pl.ds(c * step, step)
        return remote(
            extra.at[0, at], extra.at[1, at], z.across_x, ex_send.at[c], ex_recv.at[c]
        )

    def ahead_y(c):
        at = pl.ds(c * step, step)
        return remote(
            extra.at[0, at], extra.at[2, at], z.across_y, ey_send.at[c], ey_recv.at[c]
        )

    sent = []

    def go(dma):
        dma.start()
        sent.append(dma)

    go(on_x(0, me, 0))
    go(on_y(0, me, HALF))
    place = mine * GROUP + me
    for dma in norm_loads:
        dma.wait()
    size = norm_train.shape[1]
    gains[place, :, 0:size] = norms[0] + norms[1]
    passed = [pass_gains(k, place, 1) for k in range(len(z.group))]
    for i in range(2):
        for c, d in zip(EARLY, LATE):
            if i or c:
                merge(i, c)
                go(on_x(i, me, c))
                merge(i, d)
                go(on_y(i, me, d))
        for c, d in zip(EARLY, LATE):
            go(on_x(i, me, d))
            go(on_y(i, me, c))
        for c in range(CHUNKS):
            go(share(i, 0, me, c))
    for c in range(CHUNKS):
        merge(2, c)

    for dma in passed:
        dma.wait_recv()
    for k in range(len(z.group), len(peers)):
        width = 1 << (k - len(z.group))
        passed.append(pass_gains(k, lax.div(mine, width) * (width * GROUP), width * GROUP))
        passed[-1].wait_recv()
    sent += passed

    def turn(owner):
        base = pl.multiple_of(lax.div(owner, 2) * (2 * rows), LANES)

        @pl.loop(0, columns // LANES)
        def _(t):
            cols = pl.ds(pl.multiple_of(t * LANES, LANES), LANES)
            down[cols, pl.ds(base, 2 * rows)] = held[pl.ds(base, 2 * rows), cols].T

    def shared(i, slot, owner):
        for c in range(CHUNKS):
            share(i, slot, z.other_core(owner), c).wait_recv()

    for i in range(2):
        for c, d in zip(EARLY, LATE):
            on_x(i, z.across_x, c).wait_recv()
            go(forward_y(i, z.across_x, c))
            go(share(i, 1, z.across_x, c))
            on_y(i, z.across_y, d).wait_recv()
            go(forward_x(i, z.across_y, d))
            go(share(i, 2, z.across_y, d))
        if i == 1:
            @pl.when(z.core == 1)
            def _():
                for c, d in zip(EARLY, LATE):
                    ahead_x(c).start()
                    ahead_y(d).start()
                for c, d in zip(EARLY, LATE):
                    ahead_x(d).start()
                    ahead_y(c).start()
        for c, d in zip(EARLY, LATE):
            on_x(i, z.across_x, d).wait_recv()
            go(share(i, 1, z.across_x, d))
            on_y(i, z.across_y, c).wait_recv()
            go(share(i, 2, z.across_y, c))
        for slot, owner in ((0, me), (1, z.across_x), (2, z.across_y)):
            shared(i, slot, owner)
            if i == 0:
                turn(owner)
    for i in range(2):
        for c, d in zip(EARLY, LATE):
            forward_y(i, z.across, c).wait_recv()
            go(share(i, 3, z.across, c))
            forward_x(i, z.across, d).wait_recv()
            go(share(i, 3, z.across, d))
        if i == 0:
            shared(i, 3, z.across)
            turn(z.across)
    shared(1, 3, z.across)
    for dma in sent:
        dma.wait_send()

    @pl.when(z.core == 1)
    def _():
        for c in range(CHUNKS):
            ahead_x(c).wait()
            ahead_y(c).wait()


def first(sources, norms, tp):
    rows, columns = sources[0].shape
    stack = (rows * GROUP, columns)
    turned = (columns, rows * GROUP)
    dma = pltpu.SemaphoreType.DMA
    stages = GROUP - 1 + tp.bit_length() - 1
    return pl.pallas_call(
        functools.partial(first_kernel, tp),
        out_shape=(
            pltpu.VMEM(stack, jnp.bfloat16),
            pltpu.VMEM(turned, jnp.bfloat16),
            pltpu.VMEM((3, rows, columns), jnp.bfloat16),
            pltpu.VMEM((GROUP * tp, 1, LANES), jnp.float32),
        ),
        in_specs=[ANY] * 11,
        out_specs=[VMEM] * 4,
        scratch_shapes=[
            pltpu.VMEM(stack, jnp.bfloat16),
            pltpu.VMEM((3, rows, columns), jnp.bfloat16),
            pltpu.VMEM((3, *sources[1].shape), jnp.bfloat16),
            pltpu.VMEM((3, *sources[2].shape), jnp.bfloat16),
            pltpu.VMEM((2, *norms[0].shape), jnp.float32),
            dma((CHUNKS + 10,)),
            dma((stages,)), dma((stages,)),
            dma((2, CHUNKS)), dma((2, CHUNKS)), dma((2, CHUNKS)), dma((2, CHUNKS)),
            dma((2, HALF)), dma((2, HALF)), dma((2, HALF)), dma((2, HALF)),
            dma((4, 2, CHUNKS)), dma((4, 2, CHUNKS)),
            dma((CHUNKS,)), dma((CHUNKS,)), dma((CHUNKS,)), dma((CHUNKS,)),
        ],
        compiler_params=pltpu.CompilerParams(
            collective_id=0, has_side_effects=True, vmem_limit_bytes=GRANT
        ),
        name="gather_first",
    )(*sources, *norms)


def second_kernel(
    extra, after, up, ready, l_sems,
    x_send, x_recv, y_send, y_recv, fx_send, fx_recv, fy_send, fy_recv, p_send, p_recv,
):
    _, rows, columns = extra.shape
    step = rows // CHUNKS
    z = Place()
    me = z.me

    barrier = pltpu.get_barrier_semaphore()
    for peer in (z.across_x, z.across_y):
        pl.semaphore_signal(barrier, inc=1, device_id={"zero": peer}, device_id_type=MESH)

    @pl.when(z.core == 0)
    def _():
        pl.semaphore_signal(
            barrier, inc=1, device_id={"zero": z.partner}, device_id_type=MESH
        )

    pl.semaphore_wait(barrier, 2 + z.core)

    def part(owner, c):
        return up.at[pl.ds(pl.multiple_of(owner * rows + c * step, 16), step), :]

    def kept(slot, c):
        return extra.at[slot, pl.ds(c * step, step)]

    def on_x(c):
        return remote(kept(0, c), part(me, c), z.across_x, x_send.at[c], x_recv.at[c])

    def on_y(c):
        return remote(kept(0, c), part(me, c), z.across_y, y_send.at[c], y_recv.at[c])

    def forward_x(src, c):
        return remote(
            src, part(z.across_y, c), z.across_x, fx_send.at[c - HALF], fx_recv.at[c - HALF]
        )

    def forward_y(src, c):
        return remote(src, part(z.across_x, c), z.across_y, fy_send.at[c], fy_recv.at[c])

    def share(src, slot, owner, c):
        return remote(src, part(owner, c), z.partner, p_send.at[slot, c], p_recv.at[slot, c])

    def move(slot, owner):
        at = pl.ds(pl.multiple_of(owner * rows, 16), rows)
        return pltpu.make_async_copy(extra.at[slot], up.at[at, :], l_sems.at[slot])

    owners = (me, z.across_x, z.across_y)

    @pl.when(z.core == 0)
    def _():
        for c, d in zip(EARLY, LATE):
            on_x(c).start()
            on_y(d).start()
        for c, d in zip(EARLY, LATE):
            on_x(d).start()
            on_y(c).start()
        move(0, me).start()
        for c, d in zip(EARLY, LATE):
            on_x(c).wait_recv()
            forward_y(part(z.across_x, c), c).start()
            on_y(d).wait_recv()
            forward_x(part(z.across_y, d), d).start()
        for c, d in zip(EARLY, LATE):
            on_x(d).wait_recv()
            on_y(c).wait_recv()
        pl.semaphore_wait(ready, 1)
        for c in range(CHUNKS):
            share(kept(0, c), 0, me, c).start()
        for slot in (1, 2):
            for c in range(CHUNKS):
                share(part(owners[slot], c), slot, owners[slot], c).start()
        for c in range(CHUNKS):
            on_x(c).wait_send()
            on_y(c).wait_send()
        move(0, me).wait()

    @pl.when(z.core == 1)
    def _():
        pl.semaphore_signal(
            ready, inc=1, device_id={"zero": z.partner}, device_id_type=MESH
        )
        for c, d in zip(EARLY, LATE):
            forward_y(kept(1, c), c).start()
            forward_x(kept(2, d), d).start()
        for slot, owner in enumerate(owners):
            for c in range(CHUNKS):
                share(kept(slot, c), slot, owner, c).start()
        for slot, owner in enumerate(owners):
            move(slot, owner).start()
        for slot, owner in enumerate(owners):
            move(slot, owner).wait()

    for c, d in zip(EARLY, LATE):
        forward_y(kept(1, c), c).wait_recv()
        share(part(z.across, c), 3, z.across, c).start()
        forward_x(kept(2, d), d).wait_recv()
        share(part(z.across, d), 3, z.across, d).start()
    for slot, owner in enumerate((*owners, z.across)):
        for c in range(CHUNKS):
            share(part(owner, c), slot, z.other_core(owner), c).wait()
    for c, d in zip(EARLY, LATE):
        forward_y(kept(1, c), c).wait_send()
        forward_x(kept(2, d), d).wait_send()


def second(extra, after):
    _, rows, columns = extra.shape
    dma = pltpu.SemaphoreType.DMA
    extra = pltpu.with_memory_space_constraint(extra, pltpu.VMEM)
    return pl.pallas_call(
        second_kernel,
        out_shape=pltpu.VMEM((rows * GROUP, columns), jnp.bfloat16),
        in_specs=[VMEM, ANY],
        out_specs=VMEM,
        scratch_shapes=[
            pltpu.SemaphoreType.REGULAR,
            dma((3,)),
            dma((CHUNKS,)), dma((CHUNKS,)), dma((CHUNKS,)), dma((CHUNKS,)),
            dma((HALF,)), dma((HALF,)), dma((HALF,)), dma((HALF,)),
            dma((4, CHUNKS)), dma((4, CHUNKS)),
        ],
        compiler_params=pltpu.CompilerParams(
            collective_id=1, has_side_effects=True, vmem_limit_bytes=2**20
        ),
        name="gather_second",
    )(extra, after)


def start_stores(sources, targets, sems):
    pieces = 4
    copies = []
    for i, (src, dst) in enumerate(zip(sources, targets)):
        size = src.shape[0] // pieces
        for k in range(pieces):
            at = pl.ds(k * size, size)
            copies.append(pltpu.make_async_copy(src.at[at], dst.at[at], sems.at[i, k]))
            copies[-1].start()
    return copies


def store_kernel(count, *refs):
    for copy in start_stores(refs[:count], refs[count:-1], refs[-1]):
        copy.wait()


def store_norm_kernel(tp, size, gate, down, gains, gate_out, down_out, norm, lines, sems):
    copies = start_stores((gate, down), (gate_out, down_out), sems)
    lane = lax.broadcasted_iota(jnp.int32, (1, LANES), 1)
    parts = [[] for _ in range(lines.shape[0])]
    for k in range(GROUP * tp):
        zero, z = divmod(k, tp)
        piece = jnp.where(lane < size, gains[z * GROUP + zero], 0.0)
        line, shift = divmod(k * size, LANES)
        piece = pltpu.roll(piece, shift, 1) if shift else piece
        parts[line].append(jnp.where(lane >= shift, piece, 0.0))
        if shift + size > LANES:
            parts[line + 1].append(jnp.where(lane < shift, piece, 0.0))
    for line, terms in enumerate(parts):
        lines[pl.ds(line, 1), :] = sum(terms[1:], terms[0])
    norm[...] = lines[...].astype(jnp.bfloat16)
    for copy in copies:
        copy.wait()


def in_vmem(*arrays):
    return [pltpu.with_memory_space_constraint(a, pltpu.VMEM) for a in arrays]


def store(*held):
    held = in_vmem(*held)
    return pl.pallas_call(
        functools.partial(store_kernel, len(held)),
        out_shape=tuple(jax.ShapeDtypeStruct(a.shape, a.dtype) for a in held),
        in_specs=[VMEM] * len(held),
        out_specs=[ANY] * len(held),
        scratch_shapes=[pltpu.SemaphoreType.DMA((len(held), 4))],
        compiler_params=pltpu.CompilerParams(vmem_limit_bytes=2**20),
        name="store_merged",
    )(*held)


def store_norm(gate, down, gains, tp, size):
    held = in_vmem(gate, down, gains)
    lines = (GROUP * tp * size // LANES, LANES)
    shapes = [jax.ShapeDtypeStruct(a.shape, a.dtype) for a in held[:2]]
    return pl.pallas_call(
        functools.partial(store_norm_kernel, tp, size),
        out_shape=(*shapes, jax.ShapeDtypeStruct(lines, jnp.bfloat16)),
        in_specs=[VMEM] * 3,
        out_specs=[ANY, ANY, VMEM],
        scratch_shapes=[pltpu.VMEM(lines, jnp.float32), pltpu.SemaphoreType.DMA((2, 4))],
        compiler_params=pltpu.CompilerParams(vmem_limit_bytes=2**20),
        name="store_first",
    )(*held)


def local(
    weight_gate, low_gate, high_gate,
    weight_up, low_up, high_up,
    weight_down, low_down, high_down,
    norm_train, norm_step,
    *, fast, tp,
):
    sources = (
        (weight_down.T, high_down, low_down.T),
        (weight_gate, low_gate.T, high_gate),
        (weight_up, low_up.T, high_up),
    )
    if fast:
        norms = (norm_train[None], norm_step[None])
        gate, down, extra, gains = first(sum(sources, ()), norms, tp)
        ready_gate, ready_down, norm = store_norm(gate, down, gains, tp, norm_train.shape[0])
        (ready_up,) = store(second(extra, norm))
        serve_norm = norm.reshape(-1)
    else:
        down, gate, up = (merge_rows(*s) for s in sources)
        ready_gate, ready_up, ready_down = (
            lax.all_gather(a, "zero", axis=0, tiled=True) for a in (gate, up, down)
        )
        ready_down = ready_down.T
        serve_norm = lax.all_gather(
            (norm_train + norm_step).astype(jnp.bfloat16), ("zero", "tp"), axis=0, tiled=True
        )
    return (ready_gate, ready_up, ready_down, serve_norm)


def solution(mesh):
    def step(*args):
        zero, tp = mesh.shape["zero"], mesh.shape["tp"]
        rows, columns = args[0].shape[0] // zero, args[0].shape[1] // tp
        fast = (
            zero == GROUP
            and tp & (tp - 1) == 0
            and args[9].shape[0] <= zero * tp * LANES
            and args[9].shape[0] % LANES == 0
            and rows % (16 * CHUNKS) == 0
            and columns % LANES == 0
            and 2 * rows % LANES == 0
            and args[6].shape == args[0].shape[::-1]
        )
        return jax.shard_map(
            functools.partial(local, fast=fast, tp=tp),
            mesh=mesh,
            in_specs=(
                P("zero", "tp"), P("zero", None), P(None, "tp"),
                P("zero", "tp"), P("zero", None), P(None, "tp"),
                P("tp", "zero"), P("tp", None), P(None, "zero"),
                P(("zero", "tp")), P(("zero", "tp")),
            ),
            out_specs=(P(None, "tp"), P(None, "tp"), P("tp", None), P()),
            check_vma=False,
        )(*args)

    return step
```

```python
import functools

import jax
import jax.numpy as jnp
from jax import lax
from jax.experimental import pallas as pl
from jax.experimental.pallas import tpu as pltpu
from jax.sharding import PartitionSpec as P

mix_rate = 0.5
MESH = pl.DeviceIdType.MESH
LANES = 128
TILE = 2 * LANES
GROUP = 8
CHUNKS = 4
STAGES = (8, 8, 4)
COUNTS = (4, 4, 4)
PASSED = (0, 1, 2)
GRANT = 32 * 2**20
VMEM = pl.BlockSpec(memory_space=pltpu.VMEM)
ANY = pl.BlockSpec(memory_space=pl.ANY)


def merged(weight, product):
    return (weight.astype(jnp.float32) + mix_rate * product).astype(jnp.bfloat16)


def merge_rows(weight, factor, other):
    product = lax.dot_general(
        factor, other, (((0,), (0,)), ((), ())), preferred_element_type=jnp.float32
    )
    return merged(weight, product)


def stage_rows(rows):
    return [2 * rows * share // sum(STAGES) for share in STAGES]


class Place:
    def __init__(self):
        me = lax.axis_index("zero")
        core = lax.rem(me, 2)
        x = lax.rem(lax.div(me, 2), 2)
        y = lax.div(me, 4)

        def at(yy, xx, cc):
            return (yy * 2 + xx) * 2 + cc

        self.me, self.core = me, core
        self.partner = at(y, x, 1 - core)
        self.across_x = at(y, 1 - x, core)
        self.across_y = at(1 - y, x, core)
        self.across = at(1 - y, 1 - x, core)
        self.group = [
            at(
                y + dy - 2 * y * dy,
                x + dx - 2 * x * dx,
                core + dc - 2 * core * dc,
            )
            for dy in (0, 1) for dx in (0, 1) for dc in (0, 1) if dy + dx + dc
        ]

    def other_core(self, owner):
        return owner + self.partner - self.me


def remote(src, dst, peer, send, recv):
    return pltpu.make_async_remote_copy(
        src_ref=src, dst_ref=dst, send_sem=send, recv_sem=recv,
        device_id={"zero": peer}, device_id_type=MESH,
    )


class Stack:
    def __init__(self, z, part, count, sems):
        self.z, self.part, self.count, self.half = z, part, count, count // 2
        (self.x_send, self.x_recv, self.y_send, self.y_recv,
         self.fx_send, self.fx_recv, self.fy_send, self.fy_recv,
         self.p_send, self.p_recv) = sems
        self.pairs = list(zip(range(self.half), range(self.half, count)))

    @staticmethod
    def sems(count):
        dma = pltpu.SemaphoreType.DMA
        return [dma((count,))] * 4 + [dma((count // 2,))] * 4 + [dma((4, count))] * 2

    def copy(self, owner, c, peer, send, recv, src=None):
        ref = self.part(owner, c)
        return remote(ref if src is None else src, ref, peer, send, recv)

    def on_x(self, c, src=None):
        z = self.z
        return self.copy(z.me, c, z.across_x, self.x_send.at[c], self.x_recv.at[c], src)

    def on_y(self, c, src=None):
        z = self.z
        return self.copy(z.me, c, z.across_y, self.y_send.at[c], self.y_recv.at[c], src)

    def forward_x(self, c, src=None):
        z, k = self.z, c - self.half
        return self.copy(z.across_y, c, z.across_x, self.fx_send.at[k], self.fx_recv.at[k], src)

    def forward_y(self, c, src=None):
        z = self.z
        return self.copy(z.across_x, c, z.across_y, self.fy_send.at[c], self.fy_recv.at[c], src)

    def share(self, slot, owner, c, src=None):
        return self.copy(
            owner, c, self.z.partner, self.p_send.at[slot, c], self.p_recv.at[slot, c], src
        )

    def shared(self, slot, owner):
        for c in range(self.count):
            self.share(slot, owner, c).wait_recv()


class Ahead:
    def __init__(self, z, own, landed, s, sems):
        self.z, self.own, self.landed = z, own, landed
        self.count, self.step = COUNTS[s], own.shape[0] // COUNTS[s]
        (self.x_send, self.x_recv, self.y_send, self.y_recv,
         self.fx_send, self.fx_recv, self.fy_send, self.fy_recv) = sems
        self.pairs = list(zip(range(self.count // 2), range(self.count // 2, self.count)))
        self.passed = list(enumerate(self.pairs[:PASSED[s]]))

    @staticmethod
    def sems(s):
        dma = pltpu.SemaphoreType.DMA
        return [dma((COUNTS[s],))] * 4 + [dma((max(PASSED[s], 1),))] * 4

    def at(self, c):
        return pl.ds(c * self.step, self.step)

    def on_x(self, c):
        return remote(
            self.own.at[self.at(c)], self.landed.at[0, self.at(c)], self.z.across_x,
            self.x_send.at[c], self.x_recv.at[c],
        )

    def on_y(self, c):
        return remote(
            self.own.at[self.at(c)], self.landed.at[1, self.at(c)], self.z.across_y,
            self.y_send.at[c], self.y_recv.at[c],
        )

    def pass_y(self, k, c):
        return remote(
            self.landed.at[0, self.at(c)], self.landed.at[2, self.at(c)], self.z.across_y,
            self.fy_send.at[k], self.fy_recv.at[k],
        )

    def pass_x(self, k, d):
        return remote(
            self.landed.at[1, self.at(d)], self.landed.at[2, self.at(d)], self.z.across_x,
            self.fx_send.at[k], self.fx_recv.at[k],
        )

    def start(self):
        for c, d in self.pairs:
            self.on_x(c).start()
            self.on_y(d).start()
        for c, d in self.pairs:
            self.on_x(d).start()
            self.on_y(c).start()

    def finish(self):
        for k, (c, d) in self.passed:
            self.on_x(c).wait_recv()
            self.pass_y(k, c).start()
            self.on_y(d).wait_recv()
            self.pass_x(k, d).start()
        early = [c for _, (c, _) in self.passed]
        late = [d for _, (_, d) in self.passed]
        for c in range(self.count):
            self.on_x(c).wait_send()
            self.on_y(c).wait_send()
            if c not in early:
                self.on_x(c).wait_recv()
            if c not in late:
                self.on_y(c).wait_recv()
        for k, (c, d) in self.passed:
            self.pass_y(k, c).wait()
            self.pass_x(k, d).wait()


def first_kernel(tp, *refs):
    refs = list(refs)

    def take(count):
        taken, refs[:] = refs[:count], refs[count:]
        return taken

    kept = len(STAGES) - 1
    sources = [take(3) for _ in range(3)]
    norm_train, norm_step = take(2)
    block, down = take(2)
    owns = take(kept)
    landed, gains = take(2)
    held, weights, lefts, rights, norms, w_sems, n_send, n_recv = take(8)
    rows, columns = sources[1][0].shape
    step = rows // CHUNKS
    z = Place()
    me = z.me
    spans = stage_rows(rows)
    step_1 = spans[0] // COUNTS[0]

    def held_part(owner, c):
        return held.at[pl.ds(pl.multiple_of(owner * rows + c * step, 16), step), :]

    def block_part(owner, c):
        return block.at[owner, pl.ds(c * step_1, step_1)]

    stacks = (
        Stack(z, held_part, CHUNKS, take(10)), Stack(z, block_part, COUNTS[0], take(10))
    )
    ahead = Ahead(z, owns[0], landed, 1, take(8))

    mine = lax.axis_index("tp")
    peers, width = [{"zero": peer} for peer in z.group], 1
    while width < tp:
        bit = lax.rem(lax.div(mine, width), 2)
        peers.append({"tp": mine + width - 2 * width * bit})
        width *= 2

    barrier = pltpu.get_barrier_semaphore()
    for peer in peers:
        pl.semaphore_signal(barrier, inc=1, device_id=peer, device_id_type=MESH)

    loads = []

    def load(src, dst):
        loads.append(pltpu.make_async_copy(src, dst, w_sems.at[len(loads)]))
        loads[-1].start()
        return loads[-1]

    def load_narrow(i):
        _, factor, other = sources[i]
        return [load(factor, lefts.at[i]), load(other, rights.at[i])]

    order = [c for pair in stacks[0].pairs for c in pair]
    narrow = [load_narrow(0)]
    pieces = {}
    for c in order:
        at = pl.ds(c * step, step)
        pieces[c] = load(sources[0][0].at[at], weights.at[0, at])
    norm_loads = [load(norm_train, norms.at[0]), load(norm_step, norms.at[1])]
    wide = {}
    for i in (1, 2):
        narrow.append(load_narrow(i))
        wide[i] = load(sources[i][0], weights.at[i])

    turned = [None] * 3

    def merge(i, first, count, put):
        if turned[i] is None:
            for dma in narrow[i]:
                dma.wait()
            turned[i] = lefts[i].T
            if i:
                wide[i].wait()
        lhs = turned[i][first:first + count]
        for t in range(0, columns, TILE):
            cols = pl.ds(t, min(TILE, columns - t))
            product = jnp.dot(lhs, rights[i, :, cols], preferred_element_type=jnp.float32)
            put(cols, merged(weights[i, pl.ds(first, count), cols], product))

    def merge_down(c):
        pieces[c].wait()
        at = pl.ds(pl.multiple_of(me * rows + c * step, 16), step)

        def put(cols, value):
            held[at, cols] = value

        merge(0, c * step, step, put)

    def merge_stage(s, first, count):
        low = sum(spans[:s]) + first
        while count:
            i, at = 1 + low // rows, low % rows
            size = min(count, rows - at)

            def put(cols, value, first=first, size=size):
                if s:
                    owns[s - 1][pl.ds(first, size), cols] = value
                else:
                    block[me, pl.ds(first, size), cols] = value

            merge(i, at, size, put)
            low, first, count = low + size, first + size, count - size

    c, d = stacks[0].pairs[0]
    merge_down(c)
    merge_down(d)
    pl.semaphore_wait(barrier, len(peers))

    def pass_gains(k, first, count):
        part = gains.at[pl.ds(first, count)]
        dma = pltpu.make_async_remote_copy(
            src_ref=part, dst_ref=part, send_sem=n_send.at[k], recv_sem=n_recv.at[k],
            device_id=peers[k], device_id_type=MESH,
        )
        dma.start()
        return dma

    sent = []

    def go(dma):
        dma.start()
        sent.append(dma)

    go(stacks[0].on_x(c))
    go(stacks[0].on_y(d))
    place = mine * GROUP + me
    for dma in norm_loads:
        dma.wait()
    size = norm_train.shape[1]
    gains[place, :, 0:size] = norms[0] + norms[1]
    passed = [pass_gains(k, place, 1) for k in range(len(z.group))]
    for i, stack in enumerate(stacks):
        for k, (c, d) in enumerate(stack.pairs):
            if i:
                merge_stage(0, c * step_1, step_1)
                go(stack.on_x(c))
                merge_stage(0, d * step_1, step_1)
                go(stack.on_y(d))
            elif k:
                merge_down(c)
                go(stack.on_x(c))
                merge_down(d)
                go(stack.on_y(d))
        for c, d in stack.pairs:
            go(stack.on_x(d))
            go(stack.on_y(c))
        for c in range(stack.count):
            go(stack.share(0, me, c))
    for s in range(1, len(STAGES)):
        size = spans[s] // COUNTS[s]
        for c in range(COUNTS[s]):
            merge_stage(s, c * size, size)

    for dma in passed:
        dma.wait_recv()
    for k in range(len(z.group), len(peers)):
        width = 1 << (k - len(z.group))
        passed.append(pass_gains(k, lax.div(mine, width) * (width * GROUP), width * GROUP))
        passed[-1].wait_recv()
    sent += passed

    def turn(owner):
        base = pl.multiple_of(lax.div(owner, 2) * (2 * rows), LANES)

        @pl.loop(0, columns // LANES)
        def _(t):
            cols = pl.ds(pl.multiple_of(t * LANES, LANES), LANES)
            down[cols, pl.ds(base, 2 * rows)] = held[pl.ds(base, 2 * rows), cols].T

    for i, stack in enumerate(stacks):
        for c, d in stack.pairs:
            start = go if i == 0 else lambda dma: dma.start()
            stack.on_x(c).wait_recv()
            start(stack.forward_y(c))
            go(stack.share(1, z.across_x, c))
            stack.on_y(d).wait_recv()
            start(stack.forward_x(d))
            go(stack.share(2, z.across_y, d))
        for c, d in stack.pairs:
            stack.on_x(d).wait_recv()
            go(stack.share(1, z.across_x, d))
            stack.on_y(c).wait_recv()
            go(stack.share(2, z.across_y, c))
        for slot, owner in ((0, me), (1, z.across_x), (2, z.across_y)):
            stack.shared(slot, z.other_core(owner))
            if i == 0:
                turn(owner)
    for i, stack in enumerate(stacks):
        for c, d in stack.pairs:
            if i == 1 and (c, d) == stack.pairs[-1]:
                for e, f in stack.pairs:
                    stack.forward_y(e).wait_send()
                    stack.forward_x(f).wait_send()

                @pl.when(z.core == 1)
                def _():
                    ahead.start()
            stack.forward_y(c).wait_recv()
            go(stack.share(3, z.across, c))
            stack.forward_x(d).wait_recv()
            go(stack.share(3, z.across, d))
        if i == 0:
            stack.shared(3, z.other_core(z.across))
            turn(z.across)
    stacks[1].shared(3, z.other_core(z.across))
    for dma in sent:
        dma.wait_send()

    @pl.when(z.core == 1)
    def _():
        ahead.finish()


def landing(s):
    return 3 if PASSED[s] else 2


def first(sources, norms, tp):
    rows, columns = sources[0].shape
    spans = stage_rows(rows)
    dma = pltpu.SemaphoreType.DMA
    stages = GROUP - 1 + tp.bit_length() - 1
    return pl.pallas_call(
        functools.partial(first_kernel, tp),
        out_shape=(
            pltpu.VMEM((GROUP, spans[0], columns), jnp.bfloat16),
            pltpu.VMEM((columns, rows * GROUP), jnp.bfloat16),
            *(pltpu.VMEM((span, columns), jnp.bfloat16) for span in spans[1:]),
            pltpu.VMEM((landing(1), spans[1], columns), jnp.bfloat16),
            pltpu.VMEM((GROUP * tp, 1, LANES), jnp.float32),
        ),
        in_specs=[ANY] * 11,
        out_specs=[VMEM] * (len(STAGES) + 3),
        scratch_shapes=[
            pltpu.VMEM((rows * GROUP, columns), jnp.bfloat16),
            pltpu.VMEM((3, rows, columns), jnp.bfloat16),
            pltpu.VMEM((3, *sources[1].shape), jnp.bfloat16),
            pltpu.VMEM((3, *sources[2].shape), jnp.bfloat16),
            pltpu.VMEM((2, *norms[0].shape), jnp.float32),
            dma((CHUNKS + 10,)),
            dma((stages,)), dma((stages,)),
            *Stack.sems(CHUNKS), *Stack.sems(COUNTS[0]), *Ahead.sems(1),
        ],
        compiler_params=pltpu.CompilerParams(
            collective_id=0, has_side_effects=True, vmem_limit_bytes=GRANT
        ),
        name="gather_first",
    )(*sources, *norms)


def later_kernel(s, *refs):
    refs = list(refs)

    def take(count):
        taken, refs[:] = refs[:count], refs[count:]
        return taken

    last = s == len(STAGES) - 1
    own, landed, after = take(3)
    own_next = None if last else take(1)[0]
    block = take(1)[0]
    landed_next = None if last else take(1)[0]
    ready, clear, l_sems = take(3)
    count = COUNTS[s]
    step = own.shape[0] // count
    z = Place()
    me = z.me

    def part(owner, c):
        return block.at[owner, pl.ds(c * step, step)]

    stack = Stack(z, part, count, take(10))
    ahead = None if last else Ahead(z, own_next, landed_next, s + 1, take(8))
    done, rest = stack.pairs[:PASSED[s]], stack.pairs[PASSED[s]:]

    barrier = pltpu.get_barrier_semaphore()
    for peer in (z.across_x, z.across_y):
        pl.semaphore_signal(barrier, inc=1, device_id={"zero": peer}, device_id_type=MESH)

    @pl.when(z.core == 0)
    def _():
        pl.semaphore_signal(
            barrier, inc=1, device_id={"zero": z.partner}, device_id_type=MESH
        )

    pl.semaphore_wait(barrier, 2 + z.core)

    def kept(slot, c):
        at = pl.ds(c * step, step)
        return landed.at[slot - 1, at] if slot else own.at[at]

    owners = (me, z.across_x, z.across_y)

    def move(slot):
        src = landed.at[slot - 1] if slot else own
        return pltpu.make_async_copy(src, block.at[owners[slot]], l_sems.at[slot])

    def move_passed(c):
        at = pl.ds(c * step, step)
        return pltpu.make_async_copy(landed.at[2, at], part(z.across, c), l_sems.at[3 + c])

    def arrive(c, d):
        stack.forward_y(c).wait_recv()
        stack.share(3, z.across, c).start()
        stack.forward_x(d).wait_recv()
        stack.share(3, z.across, d).start()

    def sent(pairs):
        for c, d in pairs:
            stack.forward_y(c).wait_send()
            stack.forward_x(d).wait_send()

    @pl.when(z.core == 0)
    def _():
        for c, d in stack.pairs:
            stack.on_x(c, kept(0, c)).start()
            stack.on_y(d, kept(0, d)).start()
        for c, d in stack.pairs:
            stack.on_x(d, kept(0, d)).start()
            stack.on_y(c, kept(0, c)).start()
        move(0).start()
        for c, d in stack.pairs:
            stack.on_x(c).wait_recv()
            stack.forward_y(c).start()
            stack.on_y(d).wait_recv()
            stack.forward_x(d).start()
        for c, d in stack.pairs:
            stack.on_x(d).wait_recv()
            stack.on_y(c).wait_recv()
        pl.semaphore_wait(ready, 1)
        for c in range(count):
            stack.share(0, me, c, kept(0, c)).start()
        for slot in (1, 2):
            for c in range(count):
                stack.share(slot, owners[slot], c).start()
        for c in range(count):
            stack.on_x(c).wait_send()
            stack.on_y(c).wait_send()
        move(0).wait()
        for c, d in done:
            arrive(c, d)
        sent(done)

    @pl.when(z.core == 1)
    def _():
        pl.semaphore_signal(
            ready, inc=1, device_id={"zero": z.partner}, device_id_type=MESH
        )
        for c, d in rest:
            stack.forward_y(c, kept(1, c)).start()
            stack.forward_x(d, kept(2, d)).start()
        for slot, owner in enumerate(owners):
            for c in range(count):
                stack.share(slot, owner, c, kept(slot, c)).start()
        passed = [c for pair in done for c in pair]
        for c in passed:
            stack.share(3, z.across, c, landed.at[2, pl.ds(c * step, step)]).start()
        moves = [move(slot) for slot in range(3)] + [move_passed(c) for c in passed]
        for dma in moves:
            dma.start()
        for dma in moves:
            dma.wait()

    for c, d in rest[:-1]:
        arrive(c, d)
    sent(rest)
    if ahead is not None:
        @pl.when(z.core == 0)
        def _():
            pl.semaphore_signal(
                clear, inc=1, device_id={"zero": z.partner}, device_id_type=MESH
            )

        @pl.when(z.core == 1)
        def _():
            pl.semaphore_wait(clear, 1)
            ahead.start()
    for c, d in rest[-1:]:
        arrive(c, d)
    for slot, owner in enumerate((*owners, z.across)):
        stack.shared(slot, z.other_core(owner))
        for c in range(count):
            stack.share(slot, owner, c).wait_send()
    if ahead is not None:
        @pl.when(z.core == 1)
        def _():
            ahead.finish()


def in_vmem(*arrays):
    return [pltpu.with_memory_space_constraint(a, pltpu.VMEM) for a in arrays]


def later(s, owns, landed, after):
    last = s == len(STAGES) - 1
    own = owns[s - 1]
    span, columns = own.shape
    outs = [pltpu.VMEM((GROUP, span, columns), jnp.bfloat16)]
    ahead = []
    if not last:
        outs.append(pltpu.VMEM((landing(s + 1), *owns[s].shape), jnp.bfloat16))
        ahead = Ahead.sems(s + 1)
    operands = [*in_vmem(own, landed, after), *([] if last else in_vmem(owns[s]))]
    return pl.pallas_call(
        functools.partial(later_kernel, s),
        out_shape=tuple(outs),
        in_specs=[VMEM] * len(operands),
        out_specs=[VMEM] * len(outs),
        scratch_shapes=[
            pltpu.SemaphoreType.REGULAR, pltpu.SemaphoreType.REGULAR,
            pltpu.SemaphoreType.DMA((3 + COUNTS[s],)),
            *Stack.sems(COUNTS[s]), *ahead,
        ],
        compiler_params=pltpu.CompilerParams(
            collective_id=s, has_side_effects=True, vmem_limit_bytes=2**20
        ),
        name=f"gather_{s}",
    )(*operands)


def lay_norm(tp, size, gains, lines, laid):
    lane = lax.broadcasted_iota(jnp.int32, (1, LANES), 1)
    parts = [[] for _ in range(lines.shape[0])]
    for k in range(GROUP * tp):
        zero, z = divmod(k, tp)
        piece = jnp.where(lane < size, gains[z * GROUP + zero], 0.0)
        line, shift = divmod(k * size, LANES)
        piece = pltpu.roll(piece, shift, 1) if shift else piece
        parts[line].append(jnp.where(lane >= shift, piece, 0.0))
        if shift + size > LANES:
            parts[line + 1].append(jnp.where(lane < shift, piece, 0.0))
    for line, terms in enumerate(parts):
        lines[pl.ds(line, 1), :] = sum(terms[1:], terms[0])
    laid[...] = lines[...].astype(jnp.bfloat16)


def store_kernel(pieces, rows, targets, started, follows, norm_of, *refs):
    refs = list(refs)
    block = refs.pop(0)
    down = gains = None
    if norm_of:
        down, gains = refs.pop(0), refs.pop(0)
    del refs[:started]
    outs = {name: refs.pop(0) for name in targets}
    copies = []

    def go(src, dst):
        copies.append(pltpu.make_async_copy(src, dst, refs[-1].at[len(copies)]))
        copies[-1].start()

    token = refs.pop(0) if follows else None
    if norm_of:
        down_out, norm, lines, laid = (refs.pop(0) for _ in range(4))
        quarter = down.shape[0] // 4
        for k in range(4):
            at = pl.ds(k * quarter, quarter)
            go(down.at[at], down_out.at[at])
    for owner in range(GROUP):
        for name, src, dst, count in pieces:
            go(
                block.at[owner, pl.ds(src, count)],
                outs[name].at[pl.ds(owner * rows + dst, count)],
            )
    if norm_of:
        lay_norm(*norm_of, gains, lines, laid)
        go(laid, norm)
    if follows:
        token[...] = jnp.zeros_like(token)
    for copy in copies:
        copy.wait()


def store(s, block, rows, made, down=None, gains=None, tp=None, size=None):
    columns = block.shape[2]
    spans = stage_rows(rows)
    low, high = sum(spans[:s]), sum(spans[:s + 1])
    pieces = []
    for k, name in enumerate(("gate", "up")):
        a, b = max(low, k * rows), min(high, (k + 1) * rows)
        if a < b:
            pieces.append((name, a - low, a - k * rows, b - a))
    targets = [name for name, *_ in pieces]
    names = [*targets, "token"] if s < len(STAGES) - 1 else targets
    whole = jax.ShapeDtypeStruct((rows * GROUP, columns), jnp.bfloat16)
    last = s == len(STAGES) - 1
    outs = [whole] * len(targets) + [pltpu.VMEM((8, LANES), jnp.float32)] * (not last)
    operands = in_vmem(block) if down is None else in_vmem(block, down, gains)
    in_specs = [VMEM] * len(operands)
    out_specs = [ANY] * len(targets) + [VMEM] * (not last)
    aliases = {}
    for k, name in enumerate(targets):
        if name in made:
            aliases[len(operands)] = k
            operands.append(made[name])
            in_specs.append(ANY)
    copies = GROUP * len(pieces)
    scratch = []
    if down is not None:
        lines = (GROUP * tp * size // LANES, LANES)
        outs += [jax.ShapeDtypeStruct(down.shape, down.dtype),
                 jax.ShapeDtypeStruct(lines, jnp.bfloat16)]
        out_specs += [ANY, ANY]
        scratch += [pltpu.VMEM(lines, jnp.float32), pltpu.VMEM(lines, jnp.bfloat16)]
        copies += 5
        names += ["down", "norm"]
    results = pl.pallas_call(
        functools.partial(
            store_kernel, pieces, rows, targets, len(aliases), not last,
            (tp, size) if tp else None,
        ),
        out_shape=tuple(outs),
        in_specs=in_specs,
        out_specs=out_specs,
        scratch_shapes=[*scratch, pltpu.SemaphoreType.DMA((copies,))],
        input_output_aliases=aliases,
        compiler_params=pltpu.CompilerParams(vmem_limit_bytes=2**20),
        name=f"store_{s}",
    )(*operands)
    return {**made, **dict(zip(names, results))}


def local(
    weight_gate, low_gate, high_gate,
    weight_up, low_up, high_up,
    weight_down, low_down, high_down,
    norm_train, norm_step,
    *, fast, tp,
):
    sources = (
        (weight_down.T, high_down, low_down.T),
        (weight_gate, low_gate.T, high_gate),
        (weight_up, low_up.T, high_up),
    )
    if fast:
        rows = weight_gate.shape[0]
        norms = (norm_train[None], norm_step[None])
        block, down, *owns, landed, gains = first(sum(sources, ()), norms, tp)
        made = store(0, block, rows, {}, down, gains, tp, norm_train.shape[0])
        for s in range(1, len(STAGES)):
            block, *rest = later(s, owns, landed, made["token"])
            made = store(s, block, rows, made)
            landed = rest[0] if rest else None
        ready_gate, ready_up, ready_down = made["gate"], made["up"], made["down"]
        serve_norm = made["norm"].reshape(-1)
    else:
        down, gate, up = (merge_rows(*s) for s in sources)
        ready_gate, ready_up, ready_down = (
            lax.all_gather(a, "zero", axis=0, tiled=True) for a in (gate, up, down)
        )
        ready_down = ready_down.T
        serve_norm = lax.all_gather(
            (norm_train + norm_step).astype(jnp.bfloat16), ("zero", "tp"), axis=0, tiled=True
        )
    return (ready_gate, ready_up, ready_down, serve_norm)


def solution(mesh):
    def step(*args):
        zero, tp = mesh.shape["zero"], mesh.shape["tp"]
        rows, columns = args[0].shape[0] // zero, args[0].shape[1] // tp
        fast = (
            zero == GROUP
            and tp & (tp - 1) == 0
            and args[9].shape[0] <= zero * tp * LANES
            and args[9].shape[0] % LANES == 0
            and rows % (16 * CHUNKS) == 0
            and all(
                2 * rows * share % (8 * count * sum(STAGES)) == 0
                for share, count in zip(STAGES, COUNTS)
            )
            and columns % LANES == 0
            and 2 * rows % LANES == 0
            and args[6].shape == args[0].shape[::-1]
        )
        return jax.shard_map(
            functools.partial(local, fast=fast, tp=tp),
            mesh=mesh,
            in_specs=(
                P("zero", "tp"), P("zero", None), P(None, "tp"),
                P("zero", "tp"), P("zero", None), P(None, "tp"),
                P("tp", "zero"), P("tp", None), P(None, "zero"),
                P(("zero", "tp")), P(("zero", "tp")),
            ),
            out_specs=(P(None, "tp"), P(None, "tp"), P("tp", None), P()),
            check_vma=False,
        )(*args)

    return step
```

```python
import functools

import jax
import jax.numpy as jnp
from jax import lax
from jax.experimental import pallas as pl
from jax.experimental.pallas import tpu as pltpu
from jax.sharding import PartitionSpec as P

mix_rate = 0.5
MESH = pl.DeviceIdType.MESH
LANES = 128
TILE = 2 * LANES
GROUP = 8
CHUNKS = 4
STAGES = (8, 8, 4)
COUNTS = (4, 4, 4)
PASSED = (0, 1, 2)
GRANT = 32 * 2**20
VMEM = pl.BlockSpec(memory_space=pltpu.VMEM)
ANY = pl.BlockSpec(memory_space=pl.ANY)


def merged(weight, product):
    return (weight.astype(jnp.float32) + mix_rate * product).astype(jnp.bfloat16)


def merge_rows(weight, factor, other):
    product = lax.dot_general(
        factor, other, (((0,), (0,)), ((), ())), preferred_element_type=jnp.float32
    )
    return merged(weight, product)


def stage_rows(rows):
    return [2 * rows * share // sum(STAGES) for share in STAGES]


class Place:
    def __init__(self):
        me = lax.axis_index("zero")
        core = lax.rem(me, 2)
        x = lax.rem(lax.div(me, 2), 2)
        y = lax.div(me, 4)

        def at(yy, xx, cc):
            return (yy * 2 + xx) * 2 + cc

        self.me, self.core = me, core
        self.partner = at(y, x, 1 - core)
        self.across_x = at(y, 1 - x, core)
        self.across_y = at(1 - y, x, core)
        self.across = at(1 - y, 1 - x, core)
        self.group = [
            at(
                y + dy - 2 * y * dy,
                x + dx - 2 * x * dx,
                core + dc - 2 * core * dc,
            )
            for dy in (0, 1) for dx in (0, 1) for dc in (0, 1) if dy + dx + dc
        ]

    def other_core(self, owner):
        return owner + self.partner - self.me


def remote(src, dst, peer, send, recv):
    return pltpu.make_async_remote_copy(
        src_ref=src, dst_ref=dst, send_sem=send, recv_sem=recv,
        device_id={"zero": peer}, device_id_type=MESH,
    )


class Stack:
    def __init__(self, z, part, whole, count, sems):
        self.z, self.part, self.whole = z, part, whole
        self.count, self.half = count, count // 2
        self.sent, self.x, self.y, self.f_x, self.f_y, self.p = sems
        self.pairs = list(zip(range(self.half), range(self.half, count)))

    @staticmethod
    def sems(count):
        dma, half = pltpu.SemaphoreType.DMA, count // 2
        return [
            dma((3,)), dma((half + 1,)), dma((half + 1,)), dma((half,)), dma((half,)), dma((4,))
        ]

    def copy(self, owner, c, n, peer, sent, recv, src=None):
        ref = self.part(owner, c, n)
        return remote(ref if src is None else src, ref, peer, self.sent.at[sent], recv)

    def on_x(self, c, src=None):
        return self.copy(
            self.z.me, c, 1, self.z.across_x, 0, self.x.at[min(c, self.half)], src
        )

    def on_y(self, c, src=None):
        at = c - self.half if c >= self.half else self.half
        return self.copy(self.z.me, c, 1, self.z.across_y, 0, self.y.at[at], src)

    def wait_late_x(self):
        half = self.half
        self.copy(self.z.across_x, half, half, self.z.across_x, 0, self.x.at[half]).wait_recv()

    def wait_early_y(self):
        half = self.half
        self.copy(self.z.across_y, 0, half, self.z.across_y, 0, self.y.at[half]).wait_recv()

    def forward_x(self, d, src=None):
        z = self.z
        return self.copy(z.across_y, d, 1, z.across_x, 1, self.f_x.at[d - self.half], src)

    def forward_y(self, c, src=None):
        z = self.z
        return self.copy(z.across_x, c, 1, z.across_y, 1, self.f_y.at[c], src)

    def share(self, slot, owner, c, n, src=None):
        return self.copy(owner, c, n, self.z.partner, 2, self.p.at[slot], src)

    def shared(self, slot, owner):
        self.share(slot, owner, 0, self.count).wait_recv()

    def wait_sent(self, kind, ref):
        remote(ref, ref, self.z.partner, self.sent.at[kind], self.p.at[0]).wait_send()

    def wait_own(self):
        self.wait_sent(0, self.whole(2))

    def wait_forwards(self, passed=0):
        if 2 * passed < self.count:
            self.wait_sent(1, self.part(self.z.me, 0, self.count - 2 * passed))

    def wait_shares(self):
        self.wait_sent(2, self.whole(4))


class Ahead:
    def __init__(self, z, own, landed, s, sems):
        self.z, self.own, self.landed = z, own, landed
        self.count, self.step = COUNTS[s], own.shape[0] // COUNTS[s]
        self.half, self.passed = self.count // 2, PASSED[s]
        self.sent, self.x, self.y, self.f = sems

    @staticmethod
    def sems(s):
        dma = pltpu.SemaphoreType.DMA
        return [dma((2,)), dma((PASSED[s] + 1,)), dma((PASSED[s] + 1,)), dma((1,))]

    def at(self, c, n=1):
        return pl.ds(c * self.step, n * self.step)

    def on_x(self, c):
        return remote(
            self.own.at[self.at(c)], self.landed.at[0, self.at(c)], self.z.across_x,
            self.sent.at[0], self.x.at[min(c, self.passed)],
        )

    def on_y(self, c):
        k = c - self.half
        return remote(
            self.own.at[self.at(c)], self.landed.at[1, self.at(c)], self.z.across_y,
            self.sent.at[0], self.y.at[k if 0 <= k < self.passed else self.passed],
        )

    def pass_y(self, c):
        return remote(
            self.landed.at[0, self.at(c)], self.landed.at[2, self.at(c)], self.z.across_y,
            self.sent.at[1], self.f.at[0],
        )

    def pass_x(self, d):
        return remote(
            self.landed.at[1, self.at(d)], self.landed.at[2, self.at(d)], self.z.across_x,
            self.sent.at[1], self.f.at[0],
        )

    def start(self):
        half = self.half
        for c in range(half):
            self.on_x(c).start()
            self.on_y(half + c).start()
        for c in range(half):
            self.on_x(half + c).start()
            self.on_y(c).start()

    def finish(self):
        z, passed = self.z, self.passed
        for c in range(passed):
            self.on_x(c).wait_recv()
            self.pass_y(c).start()
            self.on_y(self.half + c).wait_recv()
            self.pass_x(self.half + c).start()
        both = self.landed.at[pl.ds(0, 2)]
        remote(both, both, z.across_x, self.sent.at[0], self.f.at[0]).wait_send()
        rest = self.landed.at[0, self.at(0, self.count - passed)]
        for sem in (self.x, self.y):
            remote(rest, rest, z.across_x, self.sent.at[0], sem.at[passed]).wait_recv()
        if passed:
            some = self.landed.at[2, self.at(0, 2 * passed)]
            remote(some, some, z.across_x, self.sent.at[1], self.f.at[0]).wait()


def first_kernel(tp, *refs):
    refs = list(refs)

    def take(count):
        taken, refs[:] = refs[:count], refs[count:]
        return taken

    kept = len(STAGES) - 1
    sources = [take(3) for _ in range(3)]
    norm_train, norm_step = take(2)
    block, down = take(2)
    owns = take(kept)
    landed, gains = take(2)
    held, weights, lefts, rights, norms, w_sems, n_sent, n_recv, met = take(9)
    rows, columns = sources[1][0].shape
    step = rows // CHUNKS
    z = Place()
    me = z.me
    spans = stage_rows(rows)
    step_1 = spans[0] // COUNTS[0]

    def held_part(owner, c, n):
        return held.at[pl.ds(pl.multiple_of(owner * rows + c * step, 16), n * step), :]

    def held_whole(n):
        return held.at[pl.ds(0, n * rows), :]

    def block_part(owner, c, n):
        return block.at[owner, pl.ds(c * step_1, n * step_1)]

    def block_whole(n):
        return block.at[pl.ds(0, n)]

    stacks = (
        Stack(z, held_part, held_whole, CHUNKS, take(6)),
        Stack(z, block_part, block_whole, COUNTS[0], take(6)),
    )
    ahead = Ahead(z, owns[0], landed, 1, take(4))

    mine = lax.axis_index("tp")
    near = [{"zero": peer} for peer in z.group]
    far, width = [], 1
    while width < tp:
        bit = lax.rem(lax.div(mine, width), 2)
        far.append((bit, {"tp": mine + width - 2 * width * bit}))
        width *= 2

    barrier = pltpu.get_barrier_semaphore()
    for peer in near:
        pl.semaphore_signal(barrier, inc=1, device_id=peer, device_id_type=MESH)
    for bit, peer in far:
        @pl.when(bit == 0)
        def _():
            pl.semaphore_signal(barrier, inc=1, device_id=peer, device_id_type=MESH)

    loads = []

    def load(src, dst):
        loads.append(pltpu.make_async_copy(src, dst, w_sems.at[len(loads)]))
        loads[-1].start()
        return loads[-1]

    def load_narrow(i):
        _, factor, other = sources[i]
        return [load(factor, lefts.at[i]), load(other, rights.at[i])]

    order = [c for pair in stacks[0].pairs for c in pair]
    narrow = [load_narrow(0)]
    pieces = {}
    for c in order:
        at = pl.ds(c * step, step)
        pieces[c] = load(sources[0][0].at[at], weights.at[0, at])
    norm_loads = [
        pltpu.make_async_copy(src, norms.at[k], w_sems.at[CHUNKS + 8])
        for k, src in enumerate((norm_train, norm_step))
    ]
    for dma in norm_loads:
        dma.start()
    wide = {}
    for i in (1, 2):
        narrow.append(load_narrow(i))
        wide[i] = load(sources[i][0], weights.at[i])

    turned = [None] * 3

    def merge(i, first, count, put):
        if turned[i] is None:
            for dma in narrow[i]:
                dma.wait()
            turned[i] = lefts[i].T
            if i:
                wide[i].wait()
        lhs = turned[i][first:first + count]
        for t in range(0, columns, TILE):
            cols = pl.ds(t, min(TILE, columns - t))
            product = jnp.dot(lhs, rights[i, :, cols], preferred_element_type=jnp.float32)
            put(cols, merged(weights[i, pl.ds(first, count), cols], product))

    def merge_down(c):
        pieces[c].wait()
        at = pl.ds(pl.multiple_of(me * rows + c * step, 16), step)

        def put(cols, value):
            held[at, cols] = value

        merge(0, c * step, step, put)

    def merge_stage(s, first, count):
        low = sum(spans[:s]) + first
        while count:
            i, at = 1 + low // rows, low % rows
            size = min(count, rows - at)

            def put(cols, value, first=first, size=size):
                if s:
                    owns[s - 1][pl.ds(first, size), cols] = value
                else:
                    block[me, pl.ds(first, size), cols] = value

            merge(i, at, size, put)
            low, first, count = low + size, first + size, count - size

    c, d = stacks[0].pairs[0]
    merge_down(c)
    pl.semaphore_wait(barrier, len(near) + sum(bit for bit, _ in far))
    stacks[0].on_x(c).start()
    merge_down(d)
    stacks[0].on_y(d).start()

    place = mine * GROUP + me
    pltpu.make_async_copy(norms, norms, w_sems.at[CHUNKS + 8]).wait()
    size = norm_train.shape[1]
    gains[place, :, 0:size] = norms[0] + norms[1]

    def pass_gains(k, peer, first, count):
        part = gains.at[pl.ds(first, count)]
        return pltpu.make_async_remote_copy(
            src_ref=part, dst_ref=part, send_sem=n_sent.at[0], recv_sem=n_recv.at[k],
            device_id=peer, device_id_type=MESH,
        )

    for k, peer in enumerate(near):
        pass_gains(k, peer, place, 1).start()
    for k, (bit, peer) in enumerate(far):
        @pl.when(bit == 1)
        def _():
            pl.semaphore_signal(met.at[k], inc=1, device_id=peer, device_id_type=MESH)

    for i, stack in enumerate(stacks):
        for k, (c, d) in enumerate(stack.pairs):
            if i:
                merge_stage(0, c * step_1, step_1)
                stack.on_x(c).start()
                merge_stage(0, d * step_1, step_1)
                stack.on_y(d).start()
            elif k:
                merge_down(c)
                stack.on_x(c).start()
                merge_down(d)
                stack.on_y(d).start()
        for c, d in stack.pairs:
            stack.on_x(d).start()
            stack.on_y(c).start()
        stack.share(0, me, 0, stack.count).start()
    for s in range(1, len(STAGES)):
        size = spans[s] // COUNTS[s]
        for c in range(COUNTS[s]):
            merge_stage(s, c * size, size)

    for k in range(len(near)):
        pass_gains(k, near[k], place, 1).wait_recv()
    for k, (bit, peer) in enumerate(far):
        @pl.when(bit == 0)
        def _():
            pl.semaphore_wait(met.at[k], 1)
        width = 1 << k
        dma = pass_gains(
            len(near) + k, peer, lax.div(mine, width) * (width * GROUP), width * GROUP
        )
        dma.start()
        dma.wait_recv()

    def turn(owner):
        base = pl.multiple_of(lax.div(owner, 2) * (2 * rows), LANES)

        @pl.loop(0, columns // LANES)
        def _(t):
            cols = pl.ds(pl.multiple_of(t * LANES, LANES), LANES)
            down[cols, pl.ds(base, 2 * rows)] = held[pl.ds(base, 2 * rows), cols].T

    for i, stack in enumerate(stacks):
        half = stack.half
        for c, d in stack.pairs:
            stack.on_x(c).wait_recv()
            stack.forward_y(c).start()
            stack.share(1, z.across_x, c, 1).start()
            stack.on_y(d).wait_recv()
            stack.forward_x(d).start()
            stack.share(2, z.across_y, d, 1).start()
        stack.wait_late_x()
        stack.share(1, z.across_x, half, half).start()
        stack.wait_early_y()
        stack.share(2, z.across_y, 0, half).start()
        for slot, owner in ((0, me), (1, z.across_x), (2, z.across_y)):
            stack.shared(slot, z.other_core(owner))
            if i == 0:
                turn(owner)
    for i, stack in enumerate(stacks):
        for c, d in stack.pairs:
            if i == 1 and (c, d) == stack.pairs[-1]:
                stack.wait_forwards()

                @pl.when(z.core == 1)
                def _():
                    ahead.start()
            stack.forward_y(c).wait_recv()
            stack.share(3, z.across, c, 1).start()
            stack.forward_x(d).wait_recv()
            stack.share(3, z.across, d, 1).start()
        if i == 0:
            stack.shared(3, z.other_core(z.across))
            turn(z.across)
            stack.wait_forwards()
            stack.wait_own()
            stack.wait_shares()
            done = gains.at[pl.ds(0, GROUP * tp - 1)]
            pltpu.make_async_remote_copy(
                src_ref=done, dst_ref=done, send_sem=n_sent.at[0], recv_sem=n_recv.at[0],
                device_id=near[0], device_id_type=MESH,
            ).wait_send()
    stacks[1].shared(3, z.other_core(z.across))
    stacks[1].wait_own()
    stacks[1].wait_shares()

    @pl.when(z.core == 1)
    def _():
        ahead.finish()


def landing(s):
    return 3 if PASSED[s] else 2


def first(sources, norms, tp):
    rows, columns = sources[0].shape
    spans = stage_rows(rows)
    dma = pltpu.SemaphoreType.DMA
    far = tp.bit_length() - 1
    return pl.pallas_call(
        functools.partial(first_kernel, tp),
        out_shape=(
            pltpu.VMEM((GROUP, spans[0], columns), jnp.bfloat16),
            pltpu.VMEM((columns, rows * GROUP), jnp.bfloat16),
            *(pltpu.VMEM((span, columns), jnp.bfloat16) for span in spans[1:]),
            pltpu.VMEM((landing(1), spans[1], columns), jnp.bfloat16),
            pltpu.VMEM((GROUP * tp, 1, LANES), jnp.float32),
        ),
        in_specs=[ANY] * 11,
        out_specs=[VMEM] * (len(STAGES) + 3),
        scratch_shapes=[
            pltpu.VMEM((rows * GROUP, columns), jnp.bfloat16),
            pltpu.VMEM((3, rows, columns), jnp.bfloat16),
            pltpu.VMEM((3, *sources[1].shape), jnp.bfloat16),
            pltpu.VMEM((3, *sources[2].shape), jnp.bfloat16),
            pltpu.VMEM((2, *norms[0].shape), jnp.float32),
            dma((CHUNKS + 9,)), dma((1,)), dma((GROUP - 1 + far,)),
            pltpu.SemaphoreType.REGULAR((max(far, 1),)),
            *Stack.sems(CHUNKS), *Stack.sems(COUNTS[0]), *Ahead.sems(1),
        ],
        compiler_params=pltpu.CompilerParams(
            collective_id=0, has_side_effects=True, vmem_limit_bytes=GRANT
        ),
        name="gather_first",
    )(*sources, *norms)


def later_kernel(s, *refs):
    refs = list(refs)

    def take(count):
        taken, refs[:] = refs[:count], refs[count:]
        return taken

    last = s == len(STAGES) - 1
    own, landed, after = take(3)
    own_next = None if last else take(1)[0]
    block = take(1)[0]
    landed_next = None if last else take(1)[0]
    ready, clear, l_sems = take(3)
    count = COUNTS[s]
    step = own.shape[0] // count
    z = Place()
    me = z.me

    def part(owner, c, n):
        return block.at[owner, pl.ds(c * step, n * step)]

    def whole(n):
        return block.at[pl.ds(0, n)]

    stack = Stack(z, part, whole, count, take(6))
    ahead = None if last else Ahead(z, own_next, landed_next, s + 1, take(4))
    passed = PASSED[s]
    rest = stack.pairs[passed:]

    barrier = pltpu.get_barrier_semaphore()
    for peer in (z.across_x, z.across_y):
        pl.semaphore_signal(barrier, inc=1, device_id={"zero": peer}, device_id_type=MESH)

    @pl.when(z.core == 0)
    def _():
        pl.semaphore_signal(
            barrier, inc=1, device_id={"zero": z.partner}, device_id_type=MESH
        )

    pl.semaphore_wait(barrier, 2 + z.core)

    def kept(slot, c, n):
        at = pl.ds(c * step, n * step)
        return landed.at[slot - 1, at] if slot else own.at[at]

    owners = (me, z.across_x, z.across_y)

    def move(slot):
        return pltpu.make_async_copy(kept(slot, 0, count), block.at[owners[slot]], l_sems.at[0])

    def arrive(c, d):
        stack.forward_y(c).wait_recv()
        stack.share(3, z.across, c, 1).start()
        stack.forward_x(d).wait_recv()
        stack.share(3, z.across, d, 1).start()

    @pl.when(z.core == 0)
    def _():
        for c, d in stack.pairs:
            stack.on_x(c, kept(0, c, 1)).start()
            stack.on_y(d, kept(0, d, 1)).start()
        for c, d in stack.pairs:
            stack.on_x(d, kept(0, d, 1)).start()
            stack.on_y(c, kept(0, c, 1)).start()
        move(0).start()
        for c, d in stack.pairs:
            stack.on_x(c).wait_recv()
            stack.forward_y(c).start()
            stack.on_y(d).wait_recv()
            stack.forward_x(d).start()
        stack.wait_late_x()
        stack.wait_early_y()
        pl.semaphore_wait(ready, 1)
        stack.share(0, me, 0, count, kept(0, 0, count)).start()
        for slot in (1, 2):
            stack.share(slot, owners[slot], 0, count).start()
        stack.wait_own()
        move(0).wait()
        for c, d in stack.pairs[:passed]:
            arrive(c, d)

    @pl.when(z.core == 1)
    def _():
        pl.semaphore_signal(
            ready, inc=1, device_id={"zero": z.partner}, device_id_type=MESH
        )
        for c, d in rest:
            stack.forward_y(c, kept(1, c, 1)).start()
            stack.forward_x(d, kept(2, d, 1)).start()
        for slot, owner in enumerate(owners):
            stack.share(slot, owner, 0, count, kept(slot, 0, count)).start()
        for slot in range(3):
            move(slot).start()
        for pair in stack.pairs[:passed]:
            for c in pair:
                src = landed.at[2, pl.ds(c * step, step)]
                stack.share(3, z.across, c, 1, src).start()
                pltpu.make_async_copy(src, part(z.across, c, 1), l_sems.at[1]).start()
        pltpu.make_async_copy(whole(3), whole(3), l_sems.at[0]).wait()
        if passed:
            moved = part(me, 0, 2 * passed)
            pltpu.make_async_copy(moved, moved, l_sems.at[1]).wait()

    for c, d in rest[:-1]:
        arrive(c, d)

    @pl.when(z.core == 0)
    def _():
        stack.wait_forwards()

    @pl.when(z.core == 1)
    def _():
        stack.wait_forwards(passed)

    if ahead is not None:
        @pl.when(z.core == 0)
        def _():
            pl.semaphore_signal(
                clear, inc=1, device_id={"zero": z.partner}, device_id_type=MESH
            )

        @pl.when(z.core == 1)
        def _():
            pl.semaphore_wait(clear, 1)
            ahead.start()
    for c, d in rest[-1:]:
        arrive(c, d)
    for slot, owner in enumerate((*owners, z.across)):
        stack.shared(slot, z.other_core(owner))
    stack.wait_shares()
    if ahead is not None:
        @pl.when(z.core == 1)
        def _():
            ahead.finish()


def in_vmem(*arrays):
    return [pltpu.with_memory_space_constraint(a, pltpu.VMEM) for a in arrays]


def later(s, owns, landed, after):
    last = s == len(STAGES) - 1
    own = owns[s - 1]
    span, columns = own.shape
    outs = [pltpu.VMEM((GROUP, span, columns), jnp.bfloat16)]
    ahead = []
    if not last:
        outs.append(pltpu.VMEM((landing(s + 1), *owns[s].shape), jnp.bfloat16))
        ahead = Ahead.sems(s + 1)
    operands = [*in_vmem(own, landed, after), *([] if last else in_vmem(owns[s]))]
    return pl.pallas_call(
        functools.partial(later_kernel, s),
        out_shape=tuple(outs),
        in_specs=[VMEM] * len(operands),
        out_specs=[VMEM] * len(outs),
        scratch_shapes=[
            pltpu.SemaphoreType.REGULAR, pltpu.SemaphoreType.REGULAR,
            pltpu.SemaphoreType.DMA((2,)),
            *Stack.sems(COUNTS[s]), *ahead,
        ],
        compiler_params=pltpu.CompilerParams(
            collective_id=s, has_side_effects=True, vmem_limit_bytes=2**20
        ),
        name=f"gather_{s}",
    )(*operands)


def lay_norm(tp, size, gains, lines, laid):
    lane = lax.broadcasted_iota(jnp.int32, (1, LANES), 1)
    parts = [[] for _ in range(lines.shape[0])]
    for k in range(GROUP * tp):
        zero, z = divmod(k, tp)
        piece = jnp.where(lane < size, gains[z * GROUP + zero], 0.0)
        line, shift = divmod(k * size, LANES)
        piece = pltpu.roll(piece, shift, 1) if shift else piece
        parts[line].append(jnp.where(lane >= shift, piece, 0.0))
        if shift + size > LANES:
            parts[line + 1].append(jnp.where(lane < shift, piece, 0.0))
    for line, terms in enumerate(parts):
        lines[pl.ds(line, 1), :] = sum(terms[1:], terms[0])
    laid[...] = lines[...].astype(jnp.bfloat16)


def store_kernel(pieces, rows, targets, started, follows, norm_of, *refs):
    refs = list(refs)
    block = refs.pop(0)
    down = gains = None
    if norm_of:
        down, gains = refs.pop(0), refs.pop(0)
    del refs[:started]
    outs = {name: refs.pop(0) for name in targets}
    sems = refs[-1]

    def go(src, dst, k):
        pltpu.make_async_copy(src, dst, sems.at[k]).start()

    def wait(ref, k):
        pltpu.make_async_copy(ref, ref, sems.at[k]).wait()

    token = refs.pop(0) if follows else None
    if norm_of:
        down_out, norm, lines, laid = (refs.pop(0) for _ in range(4))
        quarter = down.shape[0] // 4
        for k in range(4):
            at = pl.ds(k * quarter, quarter)
            go(down.at[at], down_out.at[at], 1)
    for owner in range(GROUP):
        for name, src, dst, count in pieces:
            go(
                block.at[owner, pl.ds(src, count)],
                outs[name].at[pl.ds(owner * rows + dst, count)],
                0,
            )
    if norm_of:
        lay_norm(*norm_of, gains, lines, laid)
        go(laid, norm, 2)
    if follows:
        token[...] = jnp.zeros_like(token)
    if norm_of:
        wait(laid, 2)
        wait(down, 1)
    wait(block, 0)


def store(s, block, rows, made, down=None, gains=None, tp=None, size=None):
    columns = block.shape[2]
    spans = stage_rows(rows)
    low, high = sum(spans[:s]), sum(spans[:s + 1])
    pieces = []
    for k, name in enumerate(("gate", "up")):
        a, b = max(low, k * rows), min(high, (k + 1) * rows)
        if a < b:
            pieces.append((name, a - low, a - k * rows, b - a))
    targets = [name for name, *_ in pieces]
    names = [*targets, "token"] if s < len(STAGES) - 1 else targets
    whole = jax.ShapeDtypeStruct((rows * GROUP, columns), jnp.bfloat16)
    last = s == len(STAGES) - 1
    outs = [whole] * len(targets) + [pltpu.VMEM((8, LANES), jnp.float32)] * (not last)
    operands = in_vmem(block) if down is None else in_vmem(block, down, gains)
    in_specs = [VMEM] * len(operands)
    out_specs = [ANY] * len(targets) + [VMEM] * (not last)
    aliases = {}
    for k, name in enumerate(targets):
        if name in made:
            aliases[len(operands)] = k
            operands.append(made[name])
            in_specs.append(ANY)
    scratch = []
    if down is not None:
        lines = (GROUP * tp * size // LANES, LANES)
        outs += [jax.ShapeDtypeStruct(down.shape, down.dtype),
                 jax.ShapeDtypeStruct(lines, jnp.bfloat16)]
        out_specs += [ANY, ANY]
        scratch += [pltpu.VMEM(lines, jnp.float32), pltpu.VMEM(lines, jnp.bfloat16)]
        names += ["down", "norm"]
    results = pl.pallas_call(
        functools.partial(
            store_kernel, pieces, rows, targets, len(aliases), not last,
            (tp, size) if tp else None,
        ),
        out_shape=tuple(outs),
        in_specs=in_specs,
        out_specs=out_specs,
        scratch_shapes=[*scratch, pltpu.SemaphoreType.DMA((3 if tp else 1,))],
        input_output_aliases=aliases,
        compiler_params=pltpu.CompilerParams(vmem_limit_bytes=2**20),
        name=f"store_{s}",
    )(*operands)
    return {**made, **dict(zip(names, results))}


def local(
    weight_gate, low_gate, high_gate,
    weight_up, low_up, high_up,
    weight_down, low_down, high_down,
    norm_train, norm_step,
    *, fast, tp,
):
    sources = (
        (weight_down.T, high_down, low_down.T),
        (weight_gate, low_gate.T, high_gate),
        (weight_up, low_up.T, high_up),
    )
    if fast:
        rows = weight_gate.shape[0]
        norms = (norm_train[None], norm_step[None])
        block, down, *owns, landed, gains = first(sum(sources, ()), norms, tp)
        made = store(0, block, rows, {}, down, gains, tp, norm_train.shape[0])
        for s in range(1, len(STAGES)):
            block, *rest = later(s, owns, landed, made["token"])
            made = store(s, block, rows, made)
            landed = rest[0] if rest else None
        ready_gate, ready_up, ready_down = made["gate"], made["up"], made["down"]
        serve_norm = made["norm"].reshape(-1)
    else:
        down, gate, up = (merge_rows(*s) for s in sources)
        ready_gate, ready_up, ready_down = (
            lax.all_gather(a, "zero", axis=0, tiled=True) for a in (gate, up, down)
        )
        ready_down = ready_down.T
        serve_norm = lax.all_gather(
            (norm_train + norm_step).astype(jnp.bfloat16), ("zero", "tp"), axis=0, tiled=True
        )
    return (ready_gate, ready_up, ready_down, serve_norm)


def solution(mesh):
    def step(*args):
        zero, tp = mesh.shape["zero"], mesh.shape["tp"]
        rows, columns = args[0].shape[0] // zero, args[0].shape[1] // tp
        fast = (
            zero == GROUP
            and tp & (tp - 1) == 0
            and args[9].shape[0] <= zero * tp * LANES
            and args[9].shape[0] % LANES == 0
            and rows % (16 * CHUNKS) == 0
            and all(
                2 * rows * share % (8 * count * sum(STAGES)) == 0
                for share, count in zip(STAGES, COUNTS)
            )
            and columns % LANES == 0
            and 2 * rows % LANES == 0
            and args[6].shape == args[0].shape[::-1]
        )
        return jax.shard_map(
            functools.partial(local, fast=fast, tp=tp),
            mesh=mesh,
            in_specs=(
                P("zero", "tp"), P("zero", None), P(None, "tp"),
                P("zero", "tp"), P("zero", None), P(None, "tp"),
                P("tp", "zero"), P("tp", None), P(None, "zero"),
                P(("zero", "tp")), P(("zero", "tp")),
            ),
            out_specs=(P(None, "tp"), P(None, "tp"), P("tp", None), P()),
            check_vma=False,
        )(*args)

    return step
```
